32 devices in a mesh: rep: 4 (over x, y), dp: 8 (over z, core).
Axes of the slice: x: 2, y: 2, z: 4, core: 2. Of those that a mesh axis runs over, the one named last changes fastest.
Arguments:
- x: bfloat16 [32, 2048, 512], P(('rep', 'dp')), parts along dimension 0
- dy: bfloat16 [32, 2048, 512], P(('rep', 'dp')), parts along dimension 0
- wq: bfloat16 [2, 512, 512], replicated
- wk: bfloat16 [2, 512, 512], replicated
- wv: bfloat16 [2, 512, 512], replicated
- wo: bfloat16 [2, 512, 512], replicated
- w_gate: bfloat16 [2, 512, 2048], replicated
- w_up: bfloat16 [2, 512, 2048], replicated
- w_down: bfloat16 [2, 2048, 512], replicated
- m_wq: float32 [2, 512, 512], P(None, 'dp')
- m_wk: float32 [2, 512, 512], P(None, 'dp')
- m_wv: float32 [2, 512, 512], P(None, 'dp')
- m_wo: float32 [2, 512, 512], P(None, 'dp')
- m_w_gate: float32 [2, 512, 2048], P(None, 'dp')
- m_w_up: float32 [2, 512, 2048], P(None, 'dp')
- m_w_down: float32 [2, 2048, 512], P(None, 'dp')
- v_wq: float32 [2, 512, 512], P(None, 'dp')
- v_wk: float32 [2, 512, 512], P(None, 'dp')
- v_wv: float32 [2, 512, 512], P(None, 'dp')
- v_wo: float32 [2, 512, 512], P(None, 'dp')
- v_w_gate: float32 [2, 512, 2048], P(None, 'dp')
- v_w_up: float32 [2, 512, 2048], P(None, 'dp')
- v_w_down: float32 [2, 2048, 512], P(None, 'dp')
Outputs:
- output 1: bfloat16 [8, 512, 512], P('rep'), parts along dimension 0
- output 2: bfloat16 [8, 512, 512], P('rep'), parts along dimension 0
- output 3: bfloat16 [8, 512, 512], P('rep'), parts along dimension 0
- output 4: bfloat16 [8, 512, 512], P('rep'), parts along dimension 0
- output 5: bfloat16 [8, 512, 2048], P('rep'), parts along dimension 0
- output 6: bfloat16 [8, 512, 2048], P('rep'), parts along dimension 0
- output 7: bfloat16 [8, 2048, 512], P('rep'), parts along dimension 0
- output 8: float32 [8, 512, 512], P('rep', 'dp'), parts along dimension 0
- output 9: float32 [8, 512, 512], P('rep', 'dp'), parts along dimension 0
- output 10: float32 [8, 512, 512], P('rep', 'dp'), parts along dimension 0
- output 11: float32 [8, 512, 512], P('rep', 'dp'), parts along dimension 0
- output 12: float32 [8, 512, 2048], P('rep', 'dp'), parts along dimension 0
- output 13: float32 [8, 512, 2048], P('rep', 'dp'), parts along dimension 0
- output 14: float32 [8, 2048, 512], P('rep', 'dp'), parts along dimension 0
- output 15: float32 [8, 512, 512], P('rep', 'dp'), parts along dimension 0
- output 16: float32 [8, 512, 512], P('rep', 'dp'), parts along dimension 0
- output 17: float32 [8, 512, 512], P('rep', 'dp'), parts along dimension 0
- output 18: float32 [8, 512, 512], P('rep', 'dp'), parts along dimension 0
- output 19: float32 [8, 512, 2048], P('rep', 'dp'), parts along dimension 0
- output 20: float32 [8, 512, 2048], P('rep', 'dp'), parts along dimension 0
- output 21: float32 [8, 2048, 512], P('rep', 'dp'), parts along dimension 0
There are 4 independent parts. The reference program is written for one: setup_inputs(seed, part) draws one part's arguments, and reference() takes and returns one part's arrays. A program takes and returns all parts, laid end to end along the dimension named above; an argument that names none is the same for every part.
All inputs are finite; a program needn't handle non-finite values.
Results may differ from the reference program's by a relative error of at most 0.024.
Values are sent between devices in bfloat16 or wider.
A program may use at most 2 GiB of HBM per device.

```python
import jax
import jax.numpy as jnp
from jax import lax

SEQUENCES = 8
TOKENS = 2048
D = 512
HEADS = 2
KV_HEADS = 2
HEAD = 256
FF = 2048
LAYERS = 2
THETA = 10000
NAMES = ("wq", "wk", "wv", "wo", "w_gate", "w_up", "w_down")
SHAPES = {
    "wq": (LAYERS, D, HEADS * HEAD),
    "wk": (LAYERS, D, KV_HEADS * HEAD),
    "wv": (LAYERS, D, KV_HEADS * HEAD),
    "wo": (LAYERS, HEADS * HEAD, D),
    "w_gate": (LAYERS, D, FF),
    "w_up": (LAYERS, D, FF),
    "w_down": (LAYERS, FF, D),
}


def bump(key, n, height):
    away = (jnp.arange(n, dtype=jnp.int32) - jax.random.randint(key, (), 0, n, jnp.int32)) % n
    return jnp.where(away < n // 8, height, 1.0)


def together(key, own, strength):
    shared = jax.random.normal(key, own.shape[1:], jnp.float32)
    return (own + strength * shared) * lax.rsqrt(1 + strength * strength)


def setup_inputs(seed: int = 0, part: int = 0) -> dict:
    kx, kdy, ka, kb, kz, kf, kh, kl, *keys = jax.random.split(jax.random.key(seed), 8 + 3 * len(NAMES))
    kx, kdy, ka, kb = (jax.random.fold_in(k, part) for k in (kx, kdy, ka, kb))
    kw, km, kv = (keys[i::3] for i in range(3))
    shape = (SEQUENCES, TOKENS, D)
    much_x, much_dy = jax.random.uniform(kz, (2,), jnp.float32, 0.0, 1.0)
    loud = 2.0 ** jax.random.uniform(jax.random.fold_in(kz, 1), (), jnp.float32, -1.0, 2.0)
    layers = 2.0 ** jax.random.uniform(kl, (LAYERS, 1, 1), jnp.float32, -1.0, 1.0)
    times = {"wq": 1.0, "wk": 1.0, "wv": 2.0, "wo": layers, "w_gate": 1.0, "w_up": bump(kh, FF, 4.0), "w_down": layers}
    x = together(ka, jax.random.normal(kx, shape, jnp.float32), much_x) * bump(kf, D, 4.0)
    dy = together(kb, jax.random.normal(kdy, shape, jnp.float32), much_dy)
    drawn = {"x": x.astype(jnp.bfloat16), "dy": (loud * dy * (SEQUENCES * TOKENS) ** -0.5).astype(jnp.bfloat16)}
    for key, name in zip(kw, NAMES, strict=True):
        drawn[name] = (jax.random.normal(key, SHAPES[name], jnp.float32) * SHAPES[name][1] ** -0.5 * times[name]).astype(jnp.bfloat16)
    for key, name in zip(km, NAMES, strict=True):
        drawn[f"m_{name}"] = 0.1 * jax.random.normal(key, SHAPES[name], jnp.float32)
    for key, name in zip(kv, NAMES, strict=True):
        drawn[f"v_{name}"] = jax.random.uniform(key, SHAPES[name], jnp.float32, 0.02, 0.06)
    return drawn


def matmul(a, w):
    return jnp.dot(a, w, preferred_element_type=jnp.float32).astype(jnp.bfloat16)


def normed(h):
    wide = h.astype(jnp.float32)
    scale = lax.rsqrt(jnp.mean(wide**2, -1, keepdims=True) + 1e-6)
    return (wide * scale).astype(jnp.bfloat16)


def turned(t, theta):
    half = t.shape[-1] // 2
    angle = jnp.arange(t.shape[0], dtype=jnp.float32)[:, None] * theta ** (-jnp.arange(half, dtype=jnp.float32) / half)
    cos, sin = jnp.cos(angle)[:, None], jnp.sin(angle)[:, None]
    a, b = t[..., :half].astype(jnp.float32), t[..., half:].astype(jnp.float32)
    return jnp.concatenate([a * cos - b * sin, b * cos + a * sin], -1).astype(jnp.bfloat16)


def seen_by(q, k, v):
    tokens, kv = q.shape[0], k.shape[1]
    q = q.reshape(tokens, kv, -1, q.shape[-1])
    scores = jnp.einsum("tgsd,ugd->gstu", q.astype(jnp.float32), k.astype(jnp.float32)) * q.shape[-1] ** -0.5
    place = jnp.arange(tokens)
    weights = jax.nn.softmax(jnp.where(place[:, None] >= place, scores, -jnp.inf), -1).astype(jnp.bfloat16)
    return jnp.einsum("gstu,ugd->tgsd", weights.astype(jnp.float32), v.astype(jnp.float32)).astype(jnp.bfloat16).reshape(tokens, -1)


def layer(h, w):
    a = normed(h)
    q, k = (turned(matmul(a, w[name]).reshape(h.shape[0], -1, HEAD), THETA) for name in ("wq", "wk"))
    h = h + matmul(seen_by(q, k, matmul(a, w["wv"]).reshape(h.shape[0], -1, HEAD)), w["wo"])
    b = normed(h)
    gate = jnp.dot(b, w["w_gate"], preferred_element_type=jnp.float32)
    up = jnp.dot(b, w["w_up"], preferred_element_type=jnp.float32)
    return h + matmul((jax.nn.silu(gate) * up).astype(jnp.bfloat16), w["w_down"])


def adamw(w, m, v, g):
    m = 0.9 * m + 0.1 * g
    v = 0.95 * v + 0.05 * g * g
    step = m * lax.rsqrt(v + 1e-8) + 0.1 * w
    return (w - 0.02 * step).astype(jnp.bfloat16), m, v


def clipped(gradients, sum_of_squares, count):
    factor = jnp.minimum(1.0, 0.5 * lax.rsqrt(sum_of_squares / count + 1e-30))
    return [g * factor for g in gradients]


def stack(weights, h):
    return lax.scan(lambda h, w: (layer(h, w), None), h, weights)[0]


def reference(x, dy, wq, wk, wv, wo, w_gate, w_up, w_down, m_wq, m_wk, m_wv, m_wo, m_w_gate, m_w_up, m_w_down, v_wq, v_wk, v_wv, v_wo, v_w_gate, v_w_up, v_w_down):
    weights = dict(zip(NAMES, (wq, wk, wv, wo, w_gate, w_up, w_down), strict=True))

    def take(so_far, sequence):
        h, by_y = sequence
        _, back = jax.vjp(stack, weights, h)
        by_weights, by_h = back(by_y)
        return jax.tree.map(lambda total, term: total + term.astype(jnp.float32), so_far, by_weights), by_h

    none_yet = {name: jnp.zeros(w.shape, jnp.float32) for name, w in weights.items()}
    by_weights, by_x = lax.scan(take, none_yet, (x, dy))
    gradients = [by_weights[name].astype(jnp.bfloat16).astype(jnp.float32) for name in NAMES]
    gradients = clipped(gradients, sum(jnp.sum(g * g) for g in gradients), sum(g.size for g in gradients))
    first = (m_wq, m_wk, m_wv, m_wo, m_w_gate, m_w_up, m_w_down)
    second = (v_wq, v_wk, v_wv, v_wo, v_w_gate, v_w_up, v_w_down)
    new = [adamw(weights[name].astype(jnp.float32), m, v, g) for name, m, v, g in zip(NAMES, first, second, gradients, strict=True)]
    return tuple(one[which] for which in range(3) for one in new)
```

```python
import functools

import jax
import jax.numpy as jnp
import numpy as np
from jax import lax
from jax.experimental import pallas as pl
from jax.experimental.pallas import tpu as pltpu
from jax.sharding import PartitionSpec as P

NEG = -1e30
HIDDEN = 2 * NEG
LOG2E = 1.4426950408889634
VMEM = 60 * 2**20
HEAD = 256
HALF = 128
THETA = 10000
TILE = 512
PART = 512
FINE = 64
NAMES = ("wq", "wk", "wv", "wo", "w_gate", "w_up", "w_down")
F32, BF16 = jnp.float32, jnp.bfloat16


def dot(a, b, ca=1, cb=0):
    return lax.dot_general(a, b, (((ca,), (cb,)), ((), ())), preferred_element_type=F32)


def rotary_tables(tokens):
    rate = float(THETA) ** (-np.arange(HALF, dtype=np.float64) / HALF)
    coarse = np.arange(0, tokens, FINE, dtype=np.float64)[:, None] * rate
    fine = np.arange(FINE, dtype=np.float64)[:, None] * rate
    return [jnp.asarray(f(t), F32) for t in (coarse, fine) for f in (np.cos, np.sin)]


def fill_rotary(tables, cos_s, sin_s):
    ca, sa, cb, sb = (t[...] for t in tables)
    for n in range(ca.shape[0]):
        c, s = ca[n : n + 1, :], sa[n : n + 1, :]
        cos_s[n * FINE : (n + 1) * FINE, :] = c * cb - s * sb
        sin_s[n * FINE : (n + 1) * FINE, :] = s * cb + c * sb


def turn(t, cos, sin):
    out = []
    for at in range(0, t.shape[1], HEAD):
        a, b = t[:, at : at + HALF], t[:, at + HALF : at + HEAD]
        out += [a * cos - b * sin, b * cos + a * sin]
    return jnp.concatenate(out, axis=1)


def norm_of(wide):
    scale = lax.rsqrt(jnp.mean(wide * wide, -1, keepdims=True) + 1e-6)
    return (wide * scale).astype(BF16), scale


def norm_back(by, wide, scale):
    along = jnp.sum(by * wide, -1, keepdims=True) * (1 / wide.shape[1])
    return (scale * by - wide * (scale * scale * scale * along)).astype(BF16)


def rounded(t):
    return t.astype(BF16).astype(F32)


def add(a, b):
    return (a.astype(F32) + b.astype(F32)).astype(BF16)


def diagonal():
    return lax.broadcasted_iota(jnp.int32, (TILE, TILE), 1) >= lax.broadcasted_iota(jnp.int32, (TILE, TILE), 0)


def forward_kernel(x_ref, ca, sa, cb, sb, wq, wk, wv, wo, wg, wu, wd, q_out, k_out, v_out, att_out, h1_out, h_out, lse_out,
                   cos_s, sin_s, h_s, k_s, vt_s, top_s, mix_s):
    layer, i = pl.program_id(0), pl.program_id(1)
    heads = wq.shape[2] // HEAD
    e = HEAD**-0.5 * LOG2E
    here = pl.ds(pl.multiple_of(i * TILE, TILE), TILE)

    @pl.when((layer == 0) & (i == 0))
    def _():
        fill_rotary((ca, sa, cb, sb), cos_s, sin_s)
        vt_s[...] = jnp.ones_like(vt_s)

    @pl.when(layer == 0)
    def _():
        h_s[here, :] = x_ref[0]

    h = h_s[here, :]
    h_out[0] = h
    a, _ = norm_of(h.astype(F32))
    cos, sin = cos_s[here, :], sin_s[here, :]
    q = turn(rounded(dot(a, wq[0])), cos, sin).astype(BF16)
    k = turn(rounded(dot(a, wk[0])), cos, sin).astype(BF16)
    v = dot(a, wv[0]).astype(BF16)
    q_out[0], k_out[0], v_out[0] = q, k, v
    k_s[here, :] = k
    vt = v.T
    for n in range(heads):
        vt_s[n, :HEAD, here] = vt[n * HEAD : (n + 1) * HEAD, :]

    top_s[...] = jnp.full_like(top_s, NEG)
    mix_s[...] = jnp.zeros_like(mix_s)

    def block(j, masked):
        at = pl.ds(pl.multiple_of(j * TILE, TILE), TILE)
        qq = q_out[0]
        scores = [dot(k_s[at, n * HEAD : (n + 1) * HEAD], qq[:, n * HEAD : (n + 1) * HEAD], 1, 1) for n in range(heads)]
        weights, keeps = [], []
        for n, s in enumerate(scores):
            if masked:
                s = jnp.where(diagonal(), s, HIDDEN)
            old = top_s[n : n + 1, :]
            top = jnp.maximum(old, s.max(axis=0, keepdims=True))
            top_s[n : n + 1, :] = top
            weights.append(jnp.exp2((s - top) * e).astype(BF16))
            keeps.append(jnp.exp2((old - top) * e))
        for n in range(heads):
            mix_s[n] = mix_s[n] * keeps[n] + dot(vt_s[n, :, at], weights[n])

    lax.fori_loop(0, i, lambda j, _: block(j, False), None)
    block(i, True)
    out = []
    for n in range(heads):
        total = mix_s[n, HEAD : HEAD + 1, :]
        out.append((mix_s[n, :HEAD, :] * (1 / total)).T.astype(BF16))
        lse_out[0, n : n + 1, :] = top_s[n : n + 1, :] * e + jnp.log2(total)
    att = jnp.concatenate(out, axis=1)
    att_out[0] = att
    h1 = add(h, dot(att, wo[0]).astype(BF16))
    h1_out[0] = h1

    @pl.when(layer < pl.num_programs(0) - 1)
    def _():
        b, _ = norm_of(h1_out[0].astype(F32))
        total = None
        for at in range(0, wg.shape[2], PART):
            gate, up = dot(b, wg[0, :, at : at + PART]), dot(b, wu[0, :, at : at + PART])
            part = dot((gate * jax.nn.sigmoid(gate) * up).astype(BF16), wd[0, at : at + PART, :])
            total = part if total is None else total + part
        h_s[here, :] = add(h1_out[0], total.astype(BF16))


def forward(x, w):
    layers, d, wide = w["wq"].shape
    tokens, hidden = x.shape[1], w["w_gate"].shape[2]
    assert tokens % TILE == 0 and hidden % PART == 0
    heads = wide // HEAD
    whole = lambda shape: pl.BlockSpec(shape, lambda l, i: (0,) * len(shape))
    each = lambda shape: pl.BlockSpec((1, *shape), lambda l, i: (l, 0, 0))
    most = lambda shape: pl.BlockSpec((1, *shape), lambda l, i: (jnp.minimum(l, layers - 2), 0, 0))
    tile = lambda width: pl.BlockSpec((1, TILE, width), lambda l, i: (l, i, 0))
    tables = rotary_tables(tokens)
    flops = 2 * tokens * (layers * d * wide * 4 + (layers - 1) * 3 * d * hidden + layers * tokens * wide)
    return pl.pallas_call(
        forward_kernel,
        grid=(layers, tokens // TILE),
        in_specs=[pl.BlockSpec((1, TILE, d), lambda l, i: (0, jnp.where(l == 0, i, tokens // TILE - 1), 0)), *(whole(t.shape) for t in tables),
                  each((d, wide)), each((d, wide)), each((d, wide)), each((wide, d)), most((d, hidden)), most((d, hidden)), most((hidden, d))],
        out_specs=[tile(wide)] * 4 + [tile(d)] * 2 + [pl.BlockSpec((1, 8, TILE), lambda l, i: (l, 0, i))],
        out_shape=[jax.ShapeDtypeStruct((layers, tokens, wide), BF16)] * 4 + [jax.ShapeDtypeStruct((layers, tokens, d), BF16)] * 2
        + [jax.ShapeDtypeStruct((layers, 8, tokens), F32)],
        scratch_shapes=[pltpu.VMEM((tokens, HALF), F32), pltpu.VMEM((tokens, HALF), F32), pltpu.VMEM((tokens, d), BF16),
                        pltpu.VMEM((tokens, wide), BF16), pltpu.VMEM((heads, HEAD + 16, tokens), BF16), pltpu.VMEM((8, TILE), F32),
                        pltpu.VMEM((heads, HEAD + 16, TILE), F32)],
        compiler_params=pltpu.CompilerParams(dimension_semantics=("arbitrary", "arbitrary"), vmem_limit_bytes=VMEM),
        cost_estimate=pl.CostEstimate(flops=flops, bytes_accessed=40 * tokens * d, transcendentals=tokens * tokens * heads),
        name="forward",
    )(x, *tables, *(w[n] for n in NAMES))


def mlp_back_kernel(by_ref, h1_ref, wg, wu, wd, by_h1, g_out, dg_s, du_s, dd_s):
    i = pl.program_id(0)
    hidden = wg.shape[2]

    @pl.when(i == 0)
    def _():
        for s in (dg_s, du_s, dd_s):
            s[...] = jnp.zeros_like(s)

    by, wide = by_ref[0], h1_ref[0].astype(F32)
    b, scale = norm_of(wide)
    bt, byt = b.T, by.T
    by_b = [None, None]
    for at in range(0, hidden, PART):
        cut = slice(at, at + PART)
        gate, up = dot(b, wg[0, :, cut]), dot(b, wu[0, :, cut])
        by_p = rounded(dot(by, wd[0, cut, :], 1, 1))
        s = jax.nn.sigmoid(gate)
        act = gate * s
        p = (act * up).astype(BF16)
        by_up = (by_p * act).astype(BF16)
        by_gate = (by_p * up * (s + act * (1 - s))).astype(BF16)
        dd_s[:, cut] += dot(byt, p)
        dg_s[:, cut] += dot(bt, by_gate)
        du_s[:, cut] += dot(bt, by_up)
        parts = dot(by_gate, wg[0, :, cut], 1, 1), dot(by_up, wu[0, :, cut], 1, 1)
        by_b = [new if old is None else old + new for old, new in zip(by_b, parts)]
    by_h1[0] = add(by, norm_back(rounded(rounded(by_b[0]) + rounded(by_b[1])), wide, scale))

    @pl.when(i == pl.num_programs(0) - 1)
    def _():
        g_out[:, :hidden] = dg_s[...].astype(BF16)
        g_out[:, hidden : 2 * hidden] = du_s[...].astype(BF16)
        d = by.shape[1]
        ways = d // ROWS
        deep = hidden // ways
        for n in range(ways):
            own = dd_s[:, n * deep : (n + 1) * deep].T.astype(BF16)
            for c in range(deep // ROWS):
                g_out[n * ROWS : (n + 1) * ROWS, 2 * hidden + c * d : 2 * hidden + (c + 1) * d] = own[c * ROWS : (c + 1) * ROWS, :]


ROWS = 64


def mlp_back(layer, at, by, h1, w):
    layers, d, hidden = w["w_gate"].shape
    tokens = by.shape[1]
    one = lambda shape: pl.BlockSpec((1, *shape), lambda i: (layer, 0, 0), pipeline_mode=pl.Buffered(1))
    tile = lambda n: pl.BlockSpec((1, TILE, d), lambda i: (n, i, 0))
    return pl.pallas_call(
        mlp_back_kernel,
        grid=(tokens // TILE,),
        in_specs=[tile(0), tile(at), one((d, hidden)), one((d, hidden)), one((hidden, d))],
        out_specs=[tile(0), pl.BlockSpec((d, 3 * hidden), lambda i: (0, 0), pipeline_mode=pl.Buffered(1))],
        out_shape=[jax.ShapeDtypeStruct((1, tokens, d), BF16), jax.ShapeDtypeStruct((d, 3 * hidden), BF16)],
        scratch_shapes=[pltpu.VMEM((d, hidden), F32)] * 3,
        compiler_params=pltpu.CompilerParams(dimension_semantics=("arbitrary",), vmem_limit_bytes=VMEM),
        cost_estimate=pl.CostEstimate(flops=16 * tokens * d * hidden, bytes_accessed=20 * tokens * d, transcendentals=tokens * hidden),
        name="mlp_back",
    )(by, h1, w["w_gate"], w["w_up"], w["w_down"])


def att_back_kernel(more, by_ref, h_ref, q_ref, k_ref, v_ref, att_ref, lse_ref, ca, sa, cb, sb, wq, wk, wv, wo, *rest):
    by_h, rest = (rest[0], rest[1:]) if more else (None, rest)
    g_out, cos_s, sin_s, dq_s, dk_s, dv_s, g_s, do_s, delta_s = rest
    step = pl.program_id(0)
    i = pl.num_programs(0) - 1 - step
    d, full = wq.shape[1], wq.shape[2]
    heads = full // HEAD
    scale = HEAD**-0.5
    e = scale * LOG2E
    here = pl.ds(pl.multiple_of(i * TILE, TILE), TILE)

    @pl.when(step == 0)
    def _():
        fill_rotary((ca, sa, cb, sb), cos_s, sin_s)
        for s in (dk_s, dv_s, g_s):
            s[...] = jnp.zeros_like(s)

    by = by_ref[0]
    by_att = dot(by, wo[0], 1, 1).astype(BF16)
    do_s[...] = by_att
    att = att_ref[0]
    g_s[3] += dot(att.T, by)
    rows = by_att.astype(F32) * att.astype(F32)
    for n in range(heads):
        delta_s[n : n + 1, :] = rows[:, n * HEAD : (n + 1) * HEAD].T.sum(axis=0, keepdims=True)
    dq_s[...] = jnp.zeros_like(dq_s)

    def block(j, masked):
        at = pl.ds(pl.multiple_of(j * TILE, TILE), TILE)
        cuts = [slice(n * HEAD, (n + 1) * HEAD) for n in range(heads)]
        qs = [q_ref[0, :, c] for c in cuts]
        dos = [do_s[:, c] for c in cuts]
        scores = [dot(k_ref[0, at, c], qs[n], 1, 1) for n, c in enumerate(cuts)]
        dps = [dot(v_ref[0, at, c], dos[n], 1, 1) for n, c in enumerate(cuts)]
        for n, c in enumerate(cuts):
            p = jnp.exp2(scores[n] * e - lse_ref[0, n : n + 1, :])
            if masked:
                p = jnp.where(diagonal(), p, 0.0)
            ds = (p * (dps[n] - delta_s[n : n + 1, :])).astype(BF16)
            dv_s[at, c] += dot(p.astype(BF16), dos[n])
            dk_s[at, c] += dot(ds, qs[n])
            dq_s[n] += dot(k_ref[0, at, c].T, ds)

    lax.fori_loop(0, i, lambda j, _: block(j, False), None)
    block(i, True)

    cos, sin = cos_s[here, :], -sin_s[here, :]
    dq = jnp.concatenate([(dq_s[n] * scale).T for n in range(heads)], axis=1)
    dq = turn(rounded(dq), cos, sin).astype(BF16)
    dk = turn(rounded(dk_s[here, :] * scale), cos, sin).astype(BF16)
    dv = dv_s[here, :].astype(BF16)
    wide = h_ref[0].astype(F32)
    a, size = norm_of(wide)
    at = a.T
    for n, t in enumerate((dq, dk, dv)):
        g_s[n] += dot(at, t)
    if more:
        by_a = sum(rounded(dot(t, m[0], 1, 1)) for t, m in ((dq, wq), (dk, wk), (dv, wv)))
        by_h[0] = add(by, norm_back(rounded(by_a), wide, size))

    @pl.when(step == pl.num_programs(0) - 1)
    def _():
        for n in range(4):
            g_out[:, n * full : (n + 1) * full] = g_s[n].astype(BF16)


def att_back(layer, by, kept, w, more):
    q, k, v, att, _, h, lse = kept
    layers, d, full = w["wq"].shape
    assert d == full
    tokens = by.shape[1]
    last = tokens // TILE - 1
    heads = full // HEAD
    whole = lambda shape: pl.BlockSpec(shape, lambda i: (0,) * len(shape))
    one = lambda shape: pl.BlockSpec((1, *shape), lambda i: (layer, 0, 0), pipeline_mode=pl.Buffered(1))
    tile = lambda n: pl.BlockSpec((1, TILE, d), lambda i: (n, last - i, 0))
    tables = rotary_tables(tokens)
    return pl.pallas_call(
        functools.partial(att_back_kernel, more),
        grid=(tokens // TILE,),
        in_specs=[tile(0), tile(layer), tile(layer), one((tokens, full)), one((tokens, full)), tile(layer),
                  pl.BlockSpec((1, 8, TILE), lambda i: (layer, 0, last - i)), *(whole(t.shape) for t in tables),
                  one((d, full)), one((d, full)), one((d, full)), one((full, d))],
        out_specs=[tile(0)] * more + [pl.BlockSpec((d, 4 * full), lambda i: (0, 0), pipeline_mode=pl.Buffered(1))],
        out_shape=[jax.ShapeDtypeStruct((1, tokens, d), BF16)] * more + [jax.ShapeDtypeStruct((d, 4 * full), BF16)],
        scratch_shapes=[pltpu.VMEM((tokens, HALF), F32), pltpu.VMEM((tokens, HALF), F32), pltpu.VMEM((heads, HEAD, TILE), F32),
                        pltpu.VMEM((tokens, full), F32), pltpu.VMEM((tokens, full), F32), pltpu.VMEM((4, d, full), F32),
                        pltpu.VMEM((TILE, full), BF16), pltpu.VMEM((8, TILE), F32)],
        compiler_params=pltpu.CompilerParams(dimension_semantics=("arbitrary",), vmem_limit_bytes=VMEM),
        cost_estimate=pl.CostEstimate(flops=2 * tokens * d * (8 * d + 3 * tokens), bytes_accessed=20 * tokens * d, transcendentals=tokens * tokens * heads // 2),
        name="att_back",
    )(by, h, q, k, v, att, lse, *tables, w["wq"], w["wk"], w["wv"], w["wo"])


def adamw(w, m, v, g):
    m = 0.9 * m + 0.1 * g
    v = 0.95 * v + 0.05 * g * g
    step = m * lax.rsqrt(v + 1e-8) + 0.1 * w
    return (w - 0.02 * step).astype(BF16), m, v


def clipped(gradients, sum_of_squares, count):
    factor = jnp.minimum(1.0, 0.5 * lax.rsqrt(sum_of_squares / count + 1e-30))
    return [g * factor for g in gradients]


def scattered(g):
    return lax.psum_scatter(g, "dp", scatter_dimension=0, tiled=True)


def solution(mesh):
    def step(x, dy, *arrays):
        weights, m, v = (arrays[i : i + 7] for i in (0, 7, 14))
        w = dict(zip(NAMES, weights, strict=True))
        layers, d, hidden = w["w_gate"].shape
        assert d == ROWS * lax.axis_size("dp")
        kept = forward(x, w)
        by, mine = dy, [None] * layers
        for n in reversed(range(layers)):
            by_h1, mlp = mlp_back(n, n, by, kept[4], w)
            mlp = scattered(mlp)
            *by_h, att = att_back(n, by_h1, kept, w, n > 0)
            att = scattered(att)
            by = by_h[0] if by_h else None
            down = jnp.concatenate([mlp[:, at : at + d] for at in range(2 * hidden, 3 * hidden, d)], axis=0)
            mine[n] = [att[:, i * d : (i + 1) * d] for i in range(4)] + [mlp[:, :hidden], mlp[:, hidden : 2 * hidden], down]
        gradients = [jnp.stack([mine[n][i] for n in range(layers)]).astype(F32) for i in range(7)]
        squares = lax.psum(sum(jnp.sum(g * g) for g in gradients), "dp")
        gradients = clipped(gradients, squares, lax.psum(1, "dp") * sum(g.size for g in gradients))
        me = lax.axis_index("dp")
        own = [lax.dynamic_slice_in_dim(w, me * one.shape[1], one.shape[1], 1).astype(F32) for w, one in zip(weights, m, strict=True)]
        new = [adamw(w, m, v, g) for w, m, v, g in zip(own, m, v, gradients, strict=True)]
        gathered = lambda ones: lax.all_gather(jnp.concatenate(ones, axis=0), "dp", axis=1, tiled=True)
        small, large = gathered([one[0] for one in new[:4]]), gathered([one[0] for one in new[4:6]])
        whole = [small[i * layers : (i + 1) * layers] for i in range(4)] + [large[i * layers : (i + 1) * layers] for i in range(2)]
        whole += [gathered([new[6][0]])]
        return (*whole, *(one[1] for one in new), *(one[2] for one in new))

    states, all_of, cut = P(("rep", "dp"), None, None), P(None, None, None), P(None, "dp", None)
    return jax.shard_map(
        step,
        mesh=mesh,
        in_specs=(states, states) + (all_of,) * 7 + (cut,) * 14,
        out_specs=(P("rep", None, None),) * 7 + (P("rep", "dp", None),) * 14,
        check_vma=False,
    )
```

```python
import functools

import jax
import jax.numpy as jnp
import numpy as np
from jax import lax
from jax.experimental import pallas as pl
from jax.experimental.pallas import tpu as pltpu
from jax.sharding import PartitionSpec as P

NEG = -1e30
HIDDEN = 2 * NEG
LOG2E = 1.4426950408889634
VMEM = 60 * 2**20
HEAD = 256
HALF = 128
THETA = 10000
TILE = 512
PART = 512
FINE = 64
NAMES = ("wq", "wk", "wv", "wo", "w_gate", "w_up", "w_down")
F32, BF16 = jnp.float32, jnp.bfloat16


def dot(a, b, ca=1, cb=0):
    return lax.dot_general(a, b, (((ca,), (cb,)), ((), ())), preferred_element_type=F32)


def rotary_tables(tokens):
    rate = float(THETA) ** (-np.arange(HALF, dtype=np.float64) / HALF)
    coarse = np.arange(0, tokens, FINE, dtype=np.float64)[:, None] * rate
    fine = np.arange(FINE, dtype=np.float64)[:, None] * rate
    return [jnp.asarray(f(t), F32) for t in (coarse, fine) for f in (np.cos, np.sin)]


def fill_rotary(tables, cos_s, sin_s):
    ca, sa, cb, sb = (t[...] for t in tables)
    for n in range(ca.shape[0]):
        c, s = ca[n : n + 1, :], sa[n : n + 1, :]
        cos_s[n * FINE : (n + 1) * FINE, :] = c * cb - s * sb
        sin_s[n * FINE : (n + 1) * FINE, :] = s * cb + c * sb


def turn(t, cos, sin):
    out = []
    for at in range(0, t.shape[1], HEAD):
        a, b = t[:, at : at + HALF], t[:, at + HALF : at + HEAD]
        out += [a * cos - b * sin, b * cos + a * sin]
    return jnp.concatenate(out, axis=1)


def norm_of(wide):
    scale = lax.rsqrt(jnp.mean(wide * wide, -1, keepdims=True) + 1e-6)
    return (wide * scale).astype(BF16), scale


def norm_back(by, wide, scale):
    along = jnp.sum(by * wide, -1, keepdims=True) * (1 / wide.shape[1])
    return (scale * by - wide * (scale * scale * scale * along)).astype(BF16)


def rounded(t):
    return t.astype(BF16).astype(F32)


def add(a, b):
    return (a.astype(F32) + b.astype(F32)).astype(BF16)


def diagonal():
    return lax.broadcasted_iota(jnp.int32, (TILE, TILE), 1) >= lax.broadcasted_iota(jnp.int32, (TILE, TILE), 0)


def forward_kernel(x_ref, ca, sa, cb, sb, wq, wk, wv, wo, wg, wu, wd, q_out, k_out, v_out, att_out, h1_out, h_out, lse_out,
                   cos_s, sin_s, h_s, k_s, vt_s, top_s, mix_s):
    layer, i = pl.program_id(0), pl.program_id(1)
    heads = wq.shape[2] // HEAD
    e = HEAD**-0.5 * LOG2E
    here = pl.ds(pl.multiple_of(i * TILE, TILE), TILE)

    @pl.when((layer == 0) & (i == 0))
    def _():
        fill_rotary((ca, sa, cb, sb), cos_s, sin_s)
        vt_s[...] = jnp.ones_like(vt_s)

    @pl.when(layer == 0)
    def _():
        h_s[here, :] = x_ref[0]

    h = h_s[here, :]
    h_out[0] = h
    a, _ = norm_of(h.astype(F32))
    cos, sin = cos_s[here, :], sin_s[here, :]
    q = turn(rounded(dot(a, wq[0])), cos, sin).astype(BF16)
    k = turn(rounded(dot(a, wk[0])), cos, sin).astype(BF16)
    v = dot(a, wv[0]).astype(BF16)
    q_out[0], k_out[0], v_out[0] = q, k, v
    k_s[here, :] = k
    vt = v.T
    for n in range(heads):
        vt_s[n, :HEAD, here] = vt[n * HEAD : (n + 1) * HEAD, :]

    top_s[...] = jnp.full_like(top_s, NEG)
    mix_s[...] = jnp.zeros_like(mix_s)

    def block(j, masked):
        at = pl.ds(pl.multiple_of(j * TILE, TILE), TILE)
        qq = q_out[0]
        scores = [dot(k_s[at, n * HEAD : (n + 1) * HEAD], qq[:, n * HEAD : (n + 1) * HEAD], 1, 1) for n in range(heads)]
        weights, keeps = [], []
        for n, s in enumerate(scores):
            if masked:
                s = jnp.where(diagonal(), s, HIDDEN)
            old = top_s[n : n + 1, :]
            top = jnp.maximum(old, s.max(axis=0, keepdims=True))
            top_s[n : n + 1, :] = top
            weights.append(jnp.exp2((s - top) * e).astype(BF16))
            keeps.append(jnp.exp2((old - top) * e))
        for n in range(heads):
            mix_s[n] = mix_s[n] * keeps[n] + dot(vt_s[n, :, at], weights[n])

    lax.fori_loop(0, i, lambda j, _: block(j, False), None)
    block(i, True)
    out = []
    for n in range(heads):
        total = mix_s[n, HEAD : HEAD + 1, :]
        out.append((mix_s[n, :HEAD, :] * (1 / total)).T.astype(BF16))
        lse_out[0, n : n + 1, :] = top_s[n : n + 1, :] * e + jnp.log2(total)
    att = jnp.concatenate(out, axis=1)
    att_out[0] = att
    h1 = add(h, dot(att, wo[0]).astype(BF16))
    h1_out[0] = h1

    @pl.when(layer < pl.num_programs(0) - 1)
    def _():
        b, _ = norm_of(h1_out[0].astype(F32))
        total = None
        for at in range(0, wg.shape[2], PART):
            gate, up = dot(b, wg[0, :, at : at + PART]), dot(b, wu[0, :, at : at + PART])
            part = dot((gate * jax.nn.sigmoid(gate) * up).astype(BF16), wd[0, at : at + PART, :])
            total = part if total is None else total + part
        h_s[here, :] = add(h1_out[0], total.astype(BF16))


def forward(x, w):
    layers, d, wide = w["wq"].shape
    tokens, hidden = x.shape[1], w["w_gate"].shape[2]
    assert tokens % TILE == 0 and hidden % PART == 0
    heads = wide // HEAD
    whole = lambda shape: pl.BlockSpec(shape, lambda l, i: (0,) * len(shape))
    each = lambda shape: pl.BlockSpec((1, *shape), lambda l, i: (l, 0, 0))
    most = lambda shape: pl.BlockSpec((1, *shape), lambda l, i: (jnp.minimum(l, layers - 2), 0, 0))
    tile = lambda width: pl.BlockSpec((1, TILE, width), lambda l, i: (l, i, 0))
    tables = rotary_tables(tokens)
    flops = 2 * tokens * (layers * d * wide * 4 + (layers - 1) * 3 * d * hidden + layers * tokens * wide)
    return pl.pallas_call(
        forward_kernel,
        grid=(layers, tokens // TILE),
        in_specs=[pl.BlockSpec((1, TILE, d), lambda l, i: (0, jnp.where(l == 0, i, tokens // TILE - 1), 0)), *(whole(t.shape) for t in tables),
                  each((d, wide)), each((d, wide)), each((d, wide)), each((wide, d)), most((d, hidden)), most((d, hidden)), most((hidden, d))],
        out_specs=[tile(wide)] * 4 + [tile(d)] * 2 + [pl.BlockSpec((1, 8, TILE), lambda l, i: (l, 0, i))],
        out_shape=[jax.ShapeDtypeStruct((layers, tokens, wide), BF16)] * 4 + [jax.ShapeDtypeStruct((layers, tokens, d), BF16)] * 2
        + [jax.ShapeDtypeStruct((layers, 8, tokens), F32)],
        scratch_shapes=[pltpu.VMEM((tokens, HALF), F32), pltpu.VMEM((tokens, HALF), F32), pltpu.VMEM((tokens, d), BF16),
                        pltpu.VMEM((tokens, wide), BF16), pltpu.VMEM((heads, HEAD + 16, tokens), BF16), pltpu.VMEM((8, TILE), F32),
                        pltpu.VMEM((heads, HEAD + 16, TILE), F32)],
        compiler_params=pltpu.CompilerParams(dimension_semantics=("arbitrary", "arbitrary"), vmem_limit_bytes=VMEM),
        cost_estimate=pl.CostEstimate(flops=flops, bytes_accessed=40 * tokens * d, transcendentals=tokens * tokens * heads),
        name="forward",
    )(x, *tables, *(w[n] for n in NAMES))


def mlp_back_kernel(by_ref, h1_ref, wg, wu, wd, by_h1, g_out, dg_s, du_s, dd_s):
    i = pl.program_id(0)
    hidden = wg.shape[2]

    @pl.when(i == 0)
    def _():
        for s in (dg_s, du_s, dd_s):
            s[...] = jnp.zeros_like(s)

    by, wide = by_ref[0], h1_ref[0].astype(F32)
    b, scale = norm_of(wide)
    bt, byt = b.T, by.T
    by_b = [None, None]
    for at in range(0, hidden, PART):
        cut = slice(at, at + PART)
        gate, up = dot(b, wg[0, :, cut]), dot(b, wu[0, :, cut])
        by_p = rounded(dot(by, wd[0, cut, :], 1, 1))
        s = jax.nn.sigmoid(gate)
        act = gate * s
        p = (act * up).astype(BF16)
        by_up = (by_p * act).astype(BF16)
        by_gate = (by_p * up * (s + act * (1 - s))).astype(BF16)
        dd_s[:, cut] += dot(byt, p)
        dg_s[:, cut] += dot(bt, by_gate)
        du_s[:, cut] += dot(bt, by_up)
        parts = dot(by_gate, wg[0, :, cut], 1, 1), dot(by_up, wu[0, :, cut], 1, 1)
        by_b = [new if old is None else old + new for old, new in zip(by_b, parts)]
    by_h1[0] = add(by, norm_back(rounded(rounded(by_b[0]) + rounded(by_b[1])), wide, scale))

    @pl.when(i == pl.num_programs(0) - 1)
    def _():
        g_out[:, :hidden] = dg_s[...].astype(BF16)
        g_out[:, hidden : 2 * hidden] = du_s[...].astype(BF16)
        d = by.shape[1]
        ways = d // ROWS
        deep = hidden // ways
        for n in range(ways):
            own = dd_s[:, n * deep : (n + 1) * deep].T.astype(BF16)
            for c in range(deep // ROWS):
                g_out[n * ROWS : (n + 1) * ROWS, 2 * hidden + c * d : 2 * hidden + (c + 1) * d] = own[c * ROWS : (c + 1) * ROWS, :]


ROWS = 64


def mlp_back(layer, at, by, h1, w):
    layers, d, hidden = w["w_gate"].shape
    tokens = by.shape[1]
    one = lambda shape: pl.BlockSpec((1, *shape), lambda i: (layer, 0, 0), pipeline_mode=pl.Buffered(1))
    tile = lambda n: pl.BlockSpec((1, TILE, d), lambda i: (n, i, 0))
    return pl.pallas_call(
        mlp_back_kernel,
        grid=(tokens // TILE,),
        in_specs=[tile(0), tile(at), one((d, hidden)), one((d, hidden)), one((hidden, d))],
        out_specs=[tile(0), pl.BlockSpec((d, 3 * hidden), lambda i: (0, 0), pipeline_mode=pl.Buffered(1))],
        out_shape=[jax.ShapeDtypeStruct((1, tokens, d), BF16), jax.ShapeDtypeStruct((d, 3 * hidden), BF16)],
        scratch_shapes=[pltpu.VMEM((d, hidden), F32)] * 3,
        compiler_params=pltpu.CompilerParams(dimension_semantics=("arbitrary",), vmem_limit_bytes=VMEM),
        cost_estimate=pl.CostEstimate(flops=16 * tokens * d * hidden, bytes_accessed=20 * tokens * d, transcendentals=tokens * hidden),
        name="mlp_back",
    )(by, h1, w["w_gate"], w["w_up"], w["w_down"])


def att_back_kernel(more, by_ref, h_ref, q_ref, k_ref, v_ref, att_ref, lse_ref, ca, sa, cb, sb, wq, wk, wv, wo, *rest):
    by_h, rest = (rest[0], rest[1:]) if more else (None, rest)
    g_out, cos_s, sin_s, dq_s, dk_s, dv_s, g_s, do_s, delta_s = rest
    step = pl.program_id(0)
    i = pl.num_programs(0) - 1 - step
    d, full = wq.shape[1], wq.shape[2]
    heads = full // HEAD
    scale = HEAD**-0.5
    e = scale * LOG2E
    here = pl.ds(pl.multiple_of(i * TILE, TILE), TILE)

    @pl.when(step == 0)
    def _():
        fill_rotary((ca, sa, cb, sb), cos_s, sin_s)
        for s in (dk_s, dv_s, g_s):
            s[...] = jnp.zeros_like(s)

    by = by_ref[0]
    by_att = dot(by, wo[0], 1, 1).astype(BF16)
    do_s[...] = by_att
    att = att_ref[0]
    g_s[3] += dot(att.T, by)
    rows = by_att.astype(F32) * att.astype(F32)
    for n in range(heads):
        delta_s[n : n + 1, :] = rows[:, n * HEAD : (n + 1) * HEAD].T.sum(axis=0, keepdims=True)
    dq_s[...] = jnp.zeros_like(dq_s)

    def block(j, masked):
        at = pl.ds(pl.multiple_of(j * TILE, TILE), TILE)
        cuts = [slice(n * HEAD, (n + 1) * HEAD) for n in range(heads)]
        qs = [q_ref[0, :, c] for c in cuts]
        dos = [do_s[:, c] for c in cuts]
        scores = [dot(k_ref[0, at, c], qs[n], 1, 1) for n, c in enumerate(cuts)]
        dps = [dot(v_ref[0, at, c], dos[n], 1, 1) for n, c in enumerate(cuts)]
        for n, c in enumerate(cuts):
            p = jnp.exp2(scores[n] * e - lse_ref[0, n : n + 1, :])
            if masked:
                p = jnp.where(diagonal(), p, 0.0)
            ds = (p * (dps[n] - delta_s[n : n + 1, :])).astype(BF16)
            dv_s[at, c] += dot(p.astype(BF16), dos[n])
            dk_s[at, c] += dot(ds, qs[n])
            dq_s[n] += dot(k_ref[0, at, c].T, ds)

    lax.fori_loop(0, i, lambda j, _: block(j, False), None)
    block(i, True)

    cos, sin = cos_s[here, :], -sin_s[here, :]
    dq = jnp.concatenate([(dq_s[n] * scale).T for n in range(heads)], axis=1)
    dq = turn(rounded(dq), cos, sin).astype(BF16)
    dk = turn(rounded(dk_s[here, :] * scale), cos, sin).astype(BF16)
    dv = dv_s[here, :].astype(BF16)
    wide = h_ref[0].astype(F32)
    a, size = norm_of(wide)
    at = a.T
    for n, t in enumerate((dq, dk, dv)):
        g_s[n] += dot(at, t)
    if more:
        by_a = sum(rounded(dot(t, m[0], 1, 1)) for t, m in ((dq, wq), (dk, wk), (dv, wv)))
        by_h[0] = add(by, norm_back(rounded(by_a), wide, size))

    @pl.when(step == pl.num_programs(0) - 1)
    def _():
        for n in range(4):
            g_out[:, n * full : (n + 1) * full] = g_s[n].astype(BF16)


def att_back(layer, by, kept, w, more):
    q, k, v, att, _, h, lse = kept
    layers, d, full = w["wq"].shape
    assert d == full
    tokens = by.shape[1]
    last = tokens // TILE - 1
    heads = full // HEAD
    whole = lambda shape: pl.BlockSpec(shape, lambda i: (0,) * len(shape))
    one = lambda shape: pl.BlockSpec((1, *shape), lambda i: (layer, 0, 0), pipeline_mode=pl.Buffered(1))
    tile = lambda n: pl.BlockSpec((1, TILE, d), lambda i: (n, last - i, 0))
    tables = rotary_tables(tokens)
    return pl.pallas_call(
        functools.partial(att_back_kernel, more),
        grid=(tokens // TILE,),
        in_specs=[tile(0), tile(layer), tile(layer), one((tokens, full)), one((tokens, full)), tile(layer),
                  pl.BlockSpec((1, 8, TILE), lambda i: (layer, 0, last - i)), *(whole(t.shape) for t in tables),
                  one((d, full)), one((d, full)), one((d, full)), one((full, d))],
        out_specs=[tile(0)] * more + [pl.BlockSpec((d, 4 * full), lambda i: (0, 0), pipeline_mode=pl.Buffered(1))],
        out_shape=[jax.ShapeDtypeStruct((1, tokens, d), BF16)] * more + [jax.ShapeDtypeStruct((d, 4 * full), BF16)],
        scratch_shapes=[pltpu.VMEM((tokens, HALF), F32), pltpu.VMEM((tokens, HALF), F32), pltpu.VMEM((heads, HEAD, TILE), F32),
                        pltpu.VMEM((tokens, full), F32), pltpu.VMEM((tokens, full), F32), pltpu.VMEM((4, d, full), F32),
                        pltpu.VMEM((TILE, full), BF16), pltpu.VMEM((8, TILE), F32)],
        compiler_params=pltpu.CompilerParams(dimension_semantics=("arbitrary",), vmem_limit_bytes=VMEM),
        cost_estimate=pl.CostEstimate(flops=2 * tokens * d * (8 * d + 3 * tokens), bytes_accessed=20 * tokens * d, transcendentals=tokens * tokens * heads // 2),
        name="att_back",
    )(by, h, q, k, v, att, lse, *tables, w["wq"], w["wk"], w["wv"], w["wo"])


LAG = 2
MESH = pl.DeviceIdType.MESH
UNIT = 512
ATT, MLP = NAMES[:4], NAMES[4:]


def units_of(names, m_shapes):
    out = []
    for name in names:
        _, rows, width = m_shapes[name]
        out += [(name, r, c) for r in range(0, rows, ROWS) for c in range(0, width, UNIT)]
    return out


def finish_kernel(places, units, ready, shapes, count, *refs):
    refs = list(refs)
    take = lambda n: [refs.pop(0) for _ in range(n)]
    raw, done = take(len(places)), take(len(ready))
    w, m, v = (dict(zip(NAMES, take(7))) for _ in range(3))
    new, m_out, v_out = (dict(zip(NAMES, take(7))) for _ in range(3))
    ws, ns, ms, vs = (dict(zip(NAMES, take(7))) for _ in range(4))
    (own, other, came, g_s, square, part, parts, own_sem, done_sem, load_sem, store_sem, psend, precv, send, recv, nsend, nrecv,
     asend, arecv) = refs
    me = lax.axis_index("dp")
    z, core = lax.div(me, 2), lax.rem(me, 2)
    partner = 2 * z + 1 - core
    left, right = jnp.maximum(me - 2, 0), jnp.minimum(me + 2, 7)
    total = sum(len(p) for p in places)
    layers = shapes["wq"][0]

    def to(src, dst, s_sem, r_sem, who):
        return pltpu.make_async_remote_copy(src_ref=src, dst_ref=dst, send_sem=s_sem, recv_sem=r_sem, device_id={"dp": who}, device_id_type=MESH)

    loads = []
    where = [(k, at) for k, p in enumerate(places) for at in range(len(p))]
    for n, (k, at) in enumerate(where):
        pltpu.make_async_copy(raw[k].at[:, core, :, pl.ds(at * UNIT, UNIT)], own.at[n], own_sem.at[n]).start()
    flat = [u for p in places for u in p]
    n = 0
    for k, p in enumerate(ready):
        for at, u in enumerate(p):
            loads.append(pltpu.make_async_copy(done[k].at[:, pl.ds(at * UNIT, UNIT)], g_s.at[u], done_sem.at[n]))
            n += 1
    for i, name in enumerate(NAMES):
        rows = shapes[name][1]
        loads.append(pltpu.make_async_copy(w[name].at[:, pl.ds(pl.multiple_of(me * rows, ROWS), rows), :], ws[name], load_sem.at[0, i]))
        loads.append(pltpu.make_async_copy(m[name], ms[name], load_sem.at[1, i]))
        loads.append(pltpu.make_async_copy(v[name], vs[name], load_sem.at[2, i]))

    barrier = pltpu.get_barrier_semaphore()
    for o in range(1, 8):
        pl.semaphore_signal(barrier, inc=1, device_id={"dp": lax.rem(me + o, 8)}, device_id_type=MESH)
    pl.semaphore_wait(barrier, 7)

    def swap(n):
        k, at = where[n]
        return to(raw[k].at[:, 1 - core, :, pl.ds(at * UNIT, UNIT)], other.at[n], psend.at[n], precv.at[n], partner)

    for n in range(total):
        swap(n).start()
    for c in loads:
        c.start()
    square[...] = jnp.zeros_like(square)

    def both(c, t):
        return own[c, t].astype(F32) + other[c, t].astype(F32)

    def hop(c, t, slot, who):
        return to(own.at[c, t], came.at[c, slot], send.at[c, t], recv.at[c, slot], who)

    def pass_on(c, t, first, slot, who):
        @pl.when(first)
        def _():
            own[c, t] = both(c, t).astype(BF16)

        @pl.when(jnp.logical_not(first))
        def _():
            hop(c, t, t, who).wait_recv()
            own[c, t] = (both(c, t) + came[c, t].astype(F32)).astype(BF16)

        hop(c, t, slot, who).start()

    def tick(t, _):
        @pl.when(t < total)
        def _():
            pltpu.make_async_copy(own.at[t], own.at[t], own_sem.at[t]).wait()
            to(own.at[t], other.at[t], psend.at[t], precv.at[t], partner).wait_recv()

        c = t - LAG * z

        @pl.when((c >= 0) & (c < total))
        def _():
            for b in (3, 2, 1):
                @pl.when(z < b)
                def _():
                    pass_on(c, b, z == 0, b, right)

        d = t - LAG * (3 - z)

        @pl.when((d >= 0) & (d < total))
        def _():
            for b in (0, 1, 2):
                @pl.when(z > b)
                def _():
                    pass_on(d, b, z == 3, jnp.where(z == b + 1, 4, b), left)

        f = t - 3 * LAG

        @pl.when(f >= 0)
        def _():
            own_part = both(f, z)

            @pl.when(z > 0)
            def _():
                hop(f, z, z, right).wait_recv()

            @pl.when(z < 3)
            def _():
                hop(f, z, 4, left).wait_recv()

            def keep(g):
                own[f, z] = g.astype(BF16)
                g = own[f, z].astype(F32)
                square[...] += g * g

            @pl.when(z == 0)
            def _():
                keep(own_part + came[f, 4].astype(F32))

            @pl.when(z == 3)
            def _():
                keep(own_part + came[f, z].astype(F32))

            @pl.when((z > 0) & (z < 3))
            def _():
                keep(own_part + came[f, z].astype(F32) + came[f, 4].astype(F32))

    lax.fori_loop(0, total + 3 * LAG, tick, None)

    def drain(c, _):
        to(own.at[c], other.at[c], psend.at[c], precv.at[c], partner).wait_send()
        for b in range(4):
            @pl.when(z != b)
            def _():
                hop(c, b, b, right).wait_send()

    lax.fori_loop(0, total, drain, None)
    for c in loads:
        c.wait()
    for p in ready:
        for u in p:
            g = g_s[u].astype(F32)
            square[...] += g * g

    part[...] = jnp.broadcast_to(jnp.sum(square[...], keepdims=True), part.shape)
    parts[me] = part[...]
    tell = [to(part, parts.at[me], nsend.at[o], nrecv.at[o], lax.rem(me + o, 8)) for o in range(1, 8)]
    for c in tell:
        c.start()
    for c in tell:
        c.wait_recv()
    size = parts[0]
    for o in range(1, 8):
        size = size + parts[o]
    factor = jnp.minimum(1.0, 0.5 * lax.rsqrt(size[:1, :1] / count + 1e-30))

    pieces = [(name, layer) for layer in reversed(range(layers)) for name in MLP] + [(name, layer) for layer in reversed(range(layers)) for name in ATT]
    spot = {u: n for n, u in enumerate(flat)}

    def region(ref, name, layer, chip, c):
        rows = shapes[name][1]
        return ref[name].at[layer, pl.ds(pl.multiple_of((2 * chip + c) * rows, ROWS), rows), :]

    def share(p, slot, chip, first, who, core_of):
        name, layer = pieces[p]
        there = region(new, name, layer, chip, core_of)
        src = ns[name].at[layer] if first else there
        return to(src, there, asend.at[slot, p], arecv.at[slot, p], who)

    stores = []
    for p in range(len(pieces) + 3):
        if p < len(pieces):
            name, layer = pieces[p]
            for u, (uname, ulayer, r, c) in enumerate(units):
                if (uname, ulayer) != (name, layer):
                    continue
                at = (layer, slice(r, r + ROWS), slice(c, c + UNIT))
                g = (own[spot[u], z] if u in spot else g_s[u]).astype(F32) * factor
                mm = 0.9 * ms[name][at] + 0.1 * g
                vv = 0.95 * vs[name][at] + 0.05 * g * g
                old = ws[name][at].astype(F32)
                ms[name][at] = mm
                vs[name][at] = vv
                ns[name][at] = (old - 0.02 * (mm * lax.rsqrt(vv + 1e-8) + 0.1 * old)).astype(BF16)

            @pl.when(z < 3)
            def _():
                share(p, 1, z, True, right, core).start()

            @pl.when(z > 0)
            def _():
                share(p, 4, z, True, left, core).start()

            share(p, 0, z, True, partner, core).start()
            stores.append(pltpu.make_async_copy(ns[name].at[layer], region(new, name, layer, z, core), store_sem.at[0, p]))
            stores.append(pltpu.make_async_copy(ms[name].at[layer], m_out[name].at[layer], store_sem.at[1, p]))
            stores.append(pltpu.make_async_copy(vs[name].at[layer], v_out[name].at[layer], store_sem.at[2, p]))
            for c in stores[-3:]:
                c.start()
        for far in (1, 2, 3):
            q = p - far
            if not 0 <= q < len(pieces):
                continue

            @pl.when(z >= far)
            def _():
                share(q, far, z - far, False, right, core).wait_recv()
                if far < 3:
                    @pl.when(z < 3)
                    def _():
                        share(q, far + 1, z - far, False, right, core).start()
                share(q, 6 + far, z - far, False, partner, core).start()

            @pl.when(z <= 3 - far)
            def _():
                share(q, 3 + far, z + far, False, left, core).wait_recv()
                if far < 3:
                    @pl.when(z > 0)
                    def _():
                        share(q, 4 + far, z + far, False, left, core).start()
                share(q, 9 + far, z + far, False, partner, core).start()

    for c in tell:
        c.wait_send()
    for p in range(len(pieces)):
        mine, theirs = share(p, 0, z, True, partner, core), share(p, 0, z, False, partner, 1 - core)
        mine.wait_send()
        theirs.wait_recv()

        @pl.when(z < 3)
        def _():
            share(p, 1, z, True, right, core).wait_send()

        @pl.when(z > 0)
        def _():
            share(p, 4, z, True, left, core).wait_send()

        for far in (1, 2, 3):
            @pl.when(z >= far)
            def _():
                if far < 3:
                    @pl.when(z < 3)
                    def _():
                        share(p, far + 1, z - far, False, right, core).wait_send()
                share(p, 6 + far, z - far, False, partner, core).wait_send()
                share(p, 6 + far, z - far, False, partner, 1 - core).wait_recv()

            @pl.when(z <= 3 - far)
            def _():
                if far < 3:
                    @pl.when(z > 0)
                    def _():
                        share(p, 4 + far, z + far, False, left, core).wait_send()
                share(p, 9 + far, z + far, False, partner, core).wait_send()
                share(p, 9 + far, z + far, False, partner, 1 - core).wait_recv()
    for c in stores:
        c.wait()


def finish(raw, ready, weights, m, v):
    shapes = {name: one.shape for name, one in zip(NAMES, m, strict=True)}
    units, cut = [], lambda layer, names: [(name, layer, r, c) for name, r, c in units_of(names, shapes)]
    places, done = [], []
    for group, out in ((raw, places), (ready, done)):
        for _, layer, names in group:
            more = cut(layer, names)
            out.append(list(range(len(units), len(units) + len(more))))
            units += more
    total, count = sum(len(p) for p in places), 8 * sum(one.size for one in m)
    any_ = pl.BlockSpec(memory_space=pl.ANY)
    own = [(one.shape, F32) for one in m]
    dma = pltpu.SemaphoreType.DMA
    layers = m[0].shape[0]
    vmem = lambda dtype: [pltpu.VMEM(shape, dtype) for shape, _ in own]
    operands = [g.reshape(4, 2, ROWS, -1) for g, _, _ in raw] + [g for g, _, _ in ready] + [*weights, *m, *v]
    got = pl.pallas_call(
        functools.partial(finish_kernel, places, units, done, shapes, count),
        in_specs=[any_] * len(operands),
        out_specs=[any_] * 21,
        out_shape=[jax.ShapeDtypeStruct(one.shape, BF16) for one in weights] + [jax.ShapeDtypeStruct(one.shape, F32) for one in (*m, *v)],
        scratch_shapes=vmem(BF16) + vmem(BF16) + vmem(F32) + vmem(F32) + [
            pltpu.VMEM((total, 4, ROWS, UNIT), BF16), pltpu.VMEM((total, 4, ROWS, UNIT), BF16), pltpu.VMEM((total, 5, ROWS, UNIT), BF16),
            pltpu.VMEM((len(units), ROWS, UNIT), BF16), pltpu.VMEM((ROWS, UNIT), F32), pltpu.VMEM((8, 128), F32), pltpu.VMEM((8, 8, 128), F32),
            dma((total,)), dma((max(len(units) - total, 1),)), dma((3, 7)), dma((3, 7 * layers)), dma((total,)), dma((total,)), dma((total, 4)), dma((total, 5)),
            dma((8,)), dma((8,)), dma((13, 7 * layers)), dma((13, 7 * layers))],
        compiler_params=pltpu.CompilerParams(collective_id=0, has_side_effects=True, vmem_limit_bytes=VMEM),
        cost_estimate=pl.CostEstimate(flops=10**9, bytes_accessed=10**8, transcendentals=0),
        name="finish",
    )(*operands)
    return got


def solution(mesh):
    def step(x, dy, *arrays):
        weights, m, v = (arrays[i : i + 7] for i in (0, 7, 14))
        w = dict(zip(NAMES, weights, strict=True))
        layers, d, _ = w["w_gate"].shape
        assert d == ROWS * lax.axis_size("dp")
        kept = forward(x, w)
        by, raw, ready = dy, [], []
        for n in reversed(range(layers)):
            by_h1, mlp = mlp_back(n, n, by, kept[4], w)
            if n > 0:
                ready.append((lax.psum_scatter(mlp, "dp", scatter_dimension=0, tiled=True), n, MLP))
            else:
                raw.append((mlp, n, MLP))
            *by_h, att = att_back(n, by_h1, kept, w, n > 0)
            raw.append((att, n, ATT))
            by = by_h[0] if by_h else None
        return tuple(finish(raw, ready, weights, m, v))

    states, all_of, cut = P(("rep", "dp"), None, None), P(None, None, None), P(None, "dp", None)
    return jax.shard_map(
        step,
        mesh=mesh,
        in_specs=(states, states) + (all_of,) * 7 + (cut,) * 14,
        out_specs=(P("rep", None, None),) * 7 + (P("rep", "dp", None),) * 14,
        check_vma=False,
    )
```

```python
import functools

import jax
import jax.numpy as jnp
import numpy as np
from jax import lax
from jax.experimental import pallas as pl
from jax.experimental.pallas import tpu as pltpu
from jax.sharding import PartitionSpec as P

NEG = -1e30
HIDDEN = 2 * NEG
LOG2E = 1.4426950408889634
VMEM = 60 * 2**20
HEAD = 256
HALF = 128
THETA = 10000
TILE = 512
PART = 512
FINE = 64
NAMES = ("wq", "wk", "wv", "wo", "w_gate", "w_up", "w_down")
F32, BF16 = jnp.float32, jnp.bfloat16


def dot(a, b, ca=1, cb=0):
    return lax.dot_general(a, b, (((ca,), (cb,)), ((), ())), preferred_element_type=F32)


def rotary_tables(tokens):
    rate = float(THETA) ** (-np.arange(HALF, dtype=np.float64) / HALF)
    coarse = np.arange(0, tokens, FINE, dtype=np.float64)[:, None] * rate
    fine = np.arange(FINE, dtype=np.float64)[:, None] * rate
    return [jnp.asarray(f(t), F32) for t in (coarse, fine) for f in (np.cos, np.sin)]


def fill_rotary(tables, cos_s, sin_s):
    ca, sa, cb, sb = (t[...] for t in tables)
    for n in range(ca.shape[0]):
        c, s = ca[n : n + 1, :], sa[n : n + 1, :]
        cos_s[n * FINE : (n + 1) * FINE, :] = c * cb - s * sb
        sin_s[n * FINE : (n + 1) * FINE, :] = s * cb + c * sb


def turn(t, cos, sin):
    out = []
    for at in range(0, t.shape[1], HEAD):
        a, b = t[:, at : at + HALF], t[:, at + HALF : at + HEAD]
        out += [a * cos - b * sin, b * cos + a * sin]
    return jnp.concatenate(out, axis=1)


def norm_of(wide):
    scale = lax.rsqrt(jnp.mean(wide * wide, -1, keepdims=True) + 1e-6)
    return (wide * scale).astype(BF16), scale


def norm_back(by, wide, scale):
    along = jnp.sum(by * wide, -1, keepdims=True) * (1 / wide.shape[1])
    return (scale * by - wide * (scale * scale * scale * along)).astype(BF16)


def rounded(t):
    return t.astype(BF16).astype(F32)


def add(a, b):
    return (a.astype(F32) + b.astype(F32)).astype(BF16)


def diagonal():
    return lax.broadcasted_iota(jnp.int32, (TILE, TILE), 1) >= lax.broadcasted_iota(jnp.int32, (TILE, TILE), 0)


LAG = 2
MESH = pl.DeviceIdType.MESH
UNIT = 512
ROWS = 64
ATT, MLP = NAMES[:4], NAMES[4:]
DMA = pltpu.SemaphoreType.DMA


def to(src, dst, s_sem, r_sem, who):
    return pltpu.make_async_remote_copy(src_ref=src, dst_ref=dst, send_sem=s_sem, recv_sem=r_sem, device_id={"dp": who}, device_id_type=MESH)


def sum_scratch(total):
    return [pltpu.VMEM((total, 4, ROWS, UNIT), BF16), pltpu.VMEM((total, 4, ROWS, UNIT), BF16), pltpu.VMEM((total, 5, ROWS, UNIT), BF16),
            DMA((total,)), DMA((total,)), DMA((total,)), DMA((total, 4)), DMA((total, 5))]


class Sum:
    def __init__(self, raw, where, scratch):
        self.raw, self.where, self.total = raw, where, len(where)
        self.ticks = self.total + 3 * LAG
        self.own, self.other, self.came, self.own_sem, self.psend, self.precv, self.send, self.recv = scratch
        self.me = lax.axis_index("dp")
        self.z, self.core = lax.div(self.me, 2), lax.rem(self.me, 2)
        self.partner = 2 * self.z + 1 - self.core
        self.left, self.right = jnp.maximum(self.me - 2, 0), jnp.minimum(self.me + 2, 7)

    def swap(self, n):
        k, at = self.where[n]
        return to(self.raw[k].at[:, 1 - self.core, :, pl.ds(at, UNIT)], self.other.at[n], self.psend.at[n], self.precv.at[n], self.partner)

    def barrier(self):
        barrier = pltpu.get_barrier_semaphore()
        for o in range(1, 8):
            pl.semaphore_signal(barrier, inc=1, device_id={"dp": lax.rem(self.me + o, 8)}, device_id_type=MESH)
        pl.semaphore_wait(barrier, 7)

    def start(self):
        for n, (k, at) in enumerate(self.where):
            pltpu.make_async_copy(self.raw[k].at[:, self.core, :, pl.ds(at, UNIT)], self.own.at[n], self.own_sem.at[n]).start()
        self.barrier()
        for n in range(self.total):
            self.swap(n).start()

    def both(self, c, t):
        return self.own[c, t].astype(F32) + self.other[c, t].astype(F32)

    def hop(self, c, t, slot, who):
        return to(self.own.at[c, t], self.came.at[c, slot], self.send.at[c, t], self.recv.at[c, slot], who)

    def pass_on(self, c, t, first, slot, who):
        @pl.when(first)
        def _():
            self.own[c, t] = self.both(c, t).astype(BF16)

        @pl.when(jnp.logical_not(first))
        def _():
            self.hop(c, t, t, who).wait_recv()
            self.own[c, t] = (self.both(c, t) + self.came[c, t].astype(F32)).astype(BF16)

        self.hop(c, t, slot, who).start()

    def tick(self, t):
        total, z = self.total, self.z

        @pl.when(t < total)
        def _():
            pltpu.make_async_copy(self.own.at[t], self.own.at[t], self.own_sem.at[t]).wait()
            to(self.own.at[t], self.other.at[t], self.psend.at[t], self.precv.at[t], self.partner).wait_recv()

        c = t - LAG * z

        @pl.when((c >= 0) & (c < total))
        def _():
            for b in (3, 2, 1):
                @pl.when(z < b)
                def _():
                    self.pass_on(c, b, z == 0, b, self.right)

        d = t - LAG * (3 - z)

        @pl.when((d >= 0) & (d < total))
        def _():
            for b in (0, 1, 2):
                @pl.when(z > b)
                def _():
                    self.pass_on(d, b, z == 3, jnp.where(z == b + 1, 4, b), self.left)

        f = t - 3 * LAG

        @pl.when((f >= 0) & (f < total))
        def _():
            @pl.when(z > 0)
            def _():
                self.hop(f, z, z, self.right).wait_recv()

            @pl.when(z < 3)
            def _():
                self.hop(f, z, 4, self.left).wait_recv()

            mine = self.both(f, z)

            @pl.when(z == 0)
            def _():
                self.own[f, z] = (mine + self.came[f, 4].astype(F32)).astype(BF16)

            @pl.when(z == 3)
            def _():
                self.own[f, z] = (mine + self.came[f, z].astype(F32)).astype(BF16)

            @pl.when((z > 0) & (z < 3))
            def _():
                self.own[f, z] = (mine + self.came[f, z].astype(F32) + self.came[f, 4].astype(F32)).astype(BF16)

    def run(self, first):
        lax.fori_loop(first, self.ticks, lambda t, _: self.tick(t), None)

    def drain(self):
        def one(c, _):
            to(self.own.at[c], self.other.at[c], self.psend.at[c], self.precv.at[c], self.partner).wait_send()
            for b in range(4):
                @pl.when(self.z != b)
                def _():
                    self.hop(c, b, b, self.right).wait_send()

        lax.fori_loop(0, self.total, one, None)

    def hand_out(self, out):
        c = pltpu.make_async_copy(self.own.at[:, self.z], out, self.own_sem.at[0])
        c.start()
        c.wait()


def forward_kernel(x_ref, ca, sa, cb, sb, wq, wk, wv, wo, wg, wu, wd, q_out, k_out, v_out, att_out, h1_out, h_out, lse_out,
                   cos_s, sin_s, h_s, k_s, vt_s, top_s, mix_s):
    layer, i = pl.program_id(0), pl.program_id(1)
    heads = wq.shape[2] // HEAD
    e = HEAD**-0.5 * LOG2E
    here = pl.ds(pl.multiple_of(i * TILE, TILE), TILE)

    @pl.when((layer == 0) & (i == 0))
    def _():
        fill_rotary((ca, sa, cb, sb), cos_s, sin_s)
        vt_s[...] = jnp.ones_like(vt_s)

    @pl.when(layer == 0)
    def _():
        h_s[here, :] = x_ref[0]

    h = h_s[here, :]
    h_out[0] = h
    a, _ = norm_of(h.astype(F32))
    cos, sin = cos_s[here, :], sin_s[here, :]
    q = turn(rounded(dot(a, wq[0])), cos, sin).astype(BF16)
    k = turn(rounded(dot(a, wk[0])), cos, sin).astype(BF16)
    v = dot(a, wv[0]).astype(BF16)
    q_out[0], k_out[0], v_out[0] = q, k, v
    k_s[here, :] = k
    vt = v.T
    for n in range(heads):
        vt_s[n, :HEAD, here] = vt[n * HEAD : (n + 1) * HEAD, :]

    top_s[...] = jnp.full_like(top_s, NEG)
    mix_s[...] = jnp.zeros_like(mix_s)

    def block(j, masked):
        at = pl.ds(pl.multiple_of(j * TILE, TILE), TILE)
        qq = q_out[0]
        scores = [dot(k_s[at, n * HEAD : (n + 1) * HEAD], qq[:, n * HEAD : (n + 1) * HEAD], 1, 1) for n in range(heads)]
        weights, keeps = [], []
        for n, s in enumerate(scores):
            if masked:
                s = jnp.where(diagonal(), s, HIDDEN)
            old = top_s[n : n + 1, :]
            top = jnp.maximum(old, s.max(axis=0, keepdims=True))
            top_s[n : n + 1, :] = top
            weights.append(jnp.exp2((s - top) * e).astype(BF16))
            keeps.append(jnp.exp2((old - top) * e))
        for n in range(heads):
            mix_s[n] = mix_s[n] * keeps[n] + dot(vt_s[n, :, at], weights[n])

    lax.fori_loop(0, i, lambda j, _: block(j, False), None)
    block(i, True)
    out = []
    for n in range(heads):
        total = mix_s[n, HEAD : HEAD + 1, :]
        out.append((mix_s[n, :HEAD, :] * (1 / total)).T.astype(BF16))
        lse_out[0, n : n + 1, :] = top_s[n : n + 1, :] * e + jnp.log2(total)
    att = jnp.concatenate(out, axis=1)
    att_out[0] = att
    h1 = add(h, dot(att, wo[0]).astype(BF16))
    h1_out[0] = h1

    @pl.when(layer < pl.num_programs(0) - 1)
    def _():
        b, _ = norm_of(h1_out[0].astype(F32))
        total = None
        for at in range(0, wg.shape[2], PART):
            gate, up = dot(b, wg[0, :, at : at + PART]), dot(b, wu[0, :, at : at + PART])
            part = dot((gate * jax.nn.sigmoid(gate) * up).astype(BF16), wd[0, at : at + PART, :])
            total = part if total is None else total + part
        h_s[here, :] = add(h1_out[0], total.astype(BF16))


def forward(x, w):
    layers, d, wide = w["wq"].shape
    tokens, hidden = x.shape[1], w["w_gate"].shape[2]
    assert tokens % TILE == 0 and hidden % PART == 0
    heads = wide // HEAD
    whole = lambda shape: pl.BlockSpec(shape, lambda l, i: (0,) * len(shape))
    each = lambda shape: pl.BlockSpec((1, *shape), lambda l, i: (l, 0, 0))
    most = lambda shape: pl.BlockSpec((1, *shape), lambda l, i: (jnp.minimum(l, layers - 2), 0, 0))
    tile = lambda width: pl.BlockSpec((1, TILE, width), lambda l, i: (l, i, 0))
    tables = rotary_tables(tokens)
    flops = 2 * tokens * (layers * d * wide * 4 + (layers - 1) * 3 * d * hidden + layers * tokens * wide)
    return pl.pallas_call(
        forward_kernel,
        grid=(layers, tokens // TILE),
        in_specs=[pl.BlockSpec((1, TILE, d), lambda l, i: (0, jnp.where(l == 0, i, tokens // TILE - 1), 0)), *(whole(t.shape) for t in tables),
                  each((d, wide)), each((d, wide)), each((d, wide)), each((wide, d)), most((d, hidden)), most((d, hidden)), most((hidden, d))],
        out_specs=[tile(wide)] * 4 + [tile(d)] * 2 + [pl.BlockSpec((1, 8, TILE), lambda l, i: (l, 0, i))],
        out_shape=[jax.ShapeDtypeStruct((layers, tokens, wide), BF16)] * 4 + [jax.ShapeDtypeStruct((layers, tokens, d), BF16)] * 2
        + [jax.ShapeDtypeStruct((layers, 8, tokens), F32)],
        scratch_shapes=[pltpu.VMEM((tokens, HALF), F32), pltpu.VMEM((tokens, HALF), F32), pltpu.VMEM((tokens, d), BF16),
                        pltpu.VMEM((tokens, wide), BF16), pltpu.VMEM((heads, HEAD + 16, tokens), BF16), pltpu.VMEM((8, TILE), F32),
                        pltpu.VMEM((heads, HEAD + 16, TILE), F32)],
        compiler_params=pltpu.CompilerParams(dimension_semantics=("arbitrary", "arbitrary"), vmem_limit_bytes=VMEM),
        cost_estimate=pl.CostEstimate(flops=flops, bytes_accessed=40 * tokens * d, transcendentals=tokens * tokens * heads),
        name="forward",
    )(x, *tables, *(w[n] for n in NAMES))


def mlp_back_kernel(where, steps, by_ref, h1_ref, wg, wu, wd, *rest):
    rest = list(rest)
    raw = [rest.pop(0) for _ in range(1 + max((n for n, _ in where), default=-1))]
    by_h1, g_out = rest.pop(0), rest.pop(0)
    summed = rest.pop(0) if where else None
    dg_s, du_s, dd_s, *rest = rest
    i = pl.program_id(0)
    hidden = wg.shape[2]
    aside = Sum(raw, where, rest) if where else None

    @pl.when(i == 0)
    def _():
        for s in (dg_s, du_s, dd_s):
            s[...] = jnp.zeros_like(s)
        if aside:
            aside.start()

    by, wide = by_ref[0], h1_ref[0].astype(F32)
    b, scale = norm_of(wide)
    bt, byt = b.T, by.T
    by_b = [None, None]
    for at in range(0, hidden, PART):
        cut = slice(at, at + PART)
        gate, up = dot(b, wg[0, :, cut]), dot(b, wu[0, :, cut])
        by_p = rounded(dot(by, wd[0, cut, :], 1, 1))
        s = jax.nn.sigmoid(gate)
        act = gate * s
        p = (act * up).astype(BF16)
        by_up = (by_p * act).astype(BF16)
        by_gate = (by_p * up * (s + act * (1 - s))).astype(BF16)
        dd_s[:, cut] += dot(byt, p)
        dg_s[:, cut] += dot(bt, by_gate)
        du_s[:, cut] += dot(bt, by_up)
        parts = dot(by_gate, wg[0, :, cut], 1, 1), dot(by_up, wu[0, :, cut], 1, 1)
        by_b = [new if old is None else old + new for old, new in zip(by_b, parts)]
        if aside:
            aside.tick(i * (hidden // PART) + at // PART)
    by_h1[0] = add(by, norm_back(rounded(rounded(by_b[0]) + rounded(by_b[1])), wide, scale))

    @pl.when(i == pl.num_programs(0) - 1)
    def _():
        g_out[:, :hidden] = dg_s[...].astype(BF16)
        g_out[:, hidden : 2 * hidden] = du_s[...].astype(BF16)
        d = by.shape[1]
        ways = d // ROWS
        deep = hidden // ways
        for n in range(ways):
            own = dd_s[:, n * deep : (n + 1) * deep].T.astype(BF16)
            for c in range(deep // ROWS):
                g_out[n * ROWS : (n + 1) * ROWS, 2 * hidden + c * d : 2 * hidden + (c + 1) * d] = own[c * ROWS : (c + 1) * ROWS, :]
        if aside:
            aside.run(steps * (hidden // PART))
            aside.drain()
            aside.hand_out(summed)


def hosted(sums):
    arrays = []
    for g, _ in sums:
        if not any(g is a for a in arrays):
            arrays.append(g)
    where = tuple(([g is a for a in arrays].index(True), at) for g, at in sums)
    any_ = pl.BlockSpec(memory_space=pl.ANY)
    if not sums:
        return [], [], [], [], [], where
    return ([g.reshape(4, 2, ROWS, -1) for g in arrays], [any_] * len(arrays), [any_], [jax.ShapeDtypeStruct((len(where), ROWS, UNIT), BF16)],
            sum_scratch(len(where)), where)


def host_params(sums, number):
    more = dict(collective_id=number, has_side_effects=True) if sums else {}
    return pltpu.CompilerParams(dimension_semantics=("arbitrary",), vmem_limit_bytes=VMEM, **more)


def mlp_back(layer, at, by, h1, w, sums=(), number=None):
    layers, d, hidden = w["w_gate"].shape
    tokens = by.shape[1]
    one = lambda shape: pl.BlockSpec((1, *shape), lambda i: (layer, 0, 0), pipeline_mode=pl.Buffered(1))
    tile = lambda n: pl.BlockSpec((1, TILE, d), lambda i: (n, i, 0))
    operands, specs, out_specs, out_shapes, scratch, where = hosted(sums)
    return pl.pallas_call(
        functools.partial(mlp_back_kernel, where, tokens // TILE),
        grid=(tokens // TILE,),
        in_specs=[tile(0), tile(at), one((d, hidden)), one((d, hidden)), one((hidden, d)), *specs],
        out_specs=[tile(0), pl.BlockSpec((d, 3 * hidden), lambda i: (0, 0), pipeline_mode=pl.Buffered(1)), *out_specs],
        out_shape=[jax.ShapeDtypeStruct((1, tokens, d), BF16), jax.ShapeDtypeStruct((d, 3 * hidden), BF16), *out_shapes],
        scratch_shapes=[pltpu.VMEM((d, hidden), F32)] * 3 + scratch,
        compiler_params=host_params(sums, number),
        cost_estimate=pl.CostEstimate(flops=16 * tokens * d * hidden, bytes_accessed=20 * tokens * d, transcendentals=tokens * hidden),
        name="mlp_back",
    )(by, h1, w["w_gate"], w["w_up"], w["w_down"], *operands)


def att_back_kernel(more, where, steps, by_ref, h_ref, q_ref, k_ref, v_ref, att_ref, lse_ref, ca, sa, cb, sb, wq, wk, wv, wo, *rest):
    rest = list(rest)
    raw = [rest.pop(0) for _ in range(1 + max((n for n, _ in where), default=-1))]
    by_h = rest.pop(0) if more else None
    g_out = rest.pop(0)
    summed = rest.pop(0) if where else None
    cos_s, sin_s, dq_s, dk_s, dv_s, g_s, do_s, delta_s, *rest = rest
    aside = Sum(raw, where, rest) if where else None
    step = pl.program_id(0)
    i = steps - 1 - step
    ticked = step * (steps + 2) - lax.div(step * (step - 1), 2)
    d, full = wq.shape[1], wq.shape[2]
    heads = full // HEAD
    scale = HEAD**-0.5
    e = scale * LOG2E
    here = pl.ds(pl.multiple_of(i * TILE, TILE), TILE)

    @pl.when(step == 0)
    def _():
        fill_rotary((ca, sa, cb, sb), cos_s, sin_s)
        for s in (dk_s, dv_s, g_s):
            s[...] = jnp.zeros_like(s)
        if aside:
            aside.start()

    by = by_ref[0]
    by_att = dot(by, wo[0], 1, 1).astype(BF16)
    do_s[...] = by_att
    att = att_ref[0]
    g_s[3] += dot(att.T, by)
    rows = by_att.astype(F32) * att.astype(F32)
    for n in range(heads):
        delta_s[n : n + 1, :] = rows[:, n * HEAD : (n + 1) * HEAD].T.sum(axis=0, keepdims=True)
    dq_s[...] = jnp.zeros_like(dq_s)
    if aside:
        aside.tick(ticked)

    def block(j, masked):
        at = pl.ds(pl.multiple_of(j * TILE, TILE), TILE)
        cuts = [slice(n * HEAD, (n + 1) * HEAD) for n in range(heads)]
        qs = [q_ref[0, :, c] for c in cuts]
        dos = [do_s[:, c] for c in cuts]
        scores = [dot(k_ref[0, at, c], qs[n], 1, 1) for n, c in enumerate(cuts)]
        dps = [dot(v_ref[0, at, c], dos[n], 1, 1) for n, c in enumerate(cuts)]
        for n, c in enumerate(cuts):
            p = jnp.exp2(scores[n] * e - lse_ref[0, n : n + 1, :])
            if masked:
                p = jnp.where(diagonal(), p, 0.0)
            ds = (p * (dps[n] - delta_s[n : n + 1, :])).astype(BF16)
            dv_s[at, c] += dot(p.astype(BF16), dos[n])
            dk_s[at, c] += dot(ds, qs[n])
            dq_s[n] += dot(k_ref[0, at, c].T, ds)
        if aside:
            aside.tick(ticked + 1 + j)

    lax.fori_loop(0, i, lambda j, _: block(j, False), None)
    block(i, True)

    cos, sin = cos_s[here, :], -sin_s[here, :]
    dq = jnp.concatenate([(dq_s[n] * scale).T for n in range(heads)], axis=1)
    dq = turn(rounded(dq), cos, sin).astype(BF16)
    dk = turn(rounded(dk_s[here, :] * scale), cos, sin).astype(BF16)
    dv = dv_s[here, :].astype(BF16)
    wide = h_ref[0].astype(F32)
    a, size = norm_of(wide)
    at = a.T
    for n, t in enumerate((dq, dk, dv)):
        g_s[n] += dot(at, t)
    if more:
        by_a = sum(rounded(dot(t, m[0], 1, 1)) for t, m in ((dq, wq), (dk, wk), (dv, wv)))
        by_h[0] = add(by, norm_back(rounded(by_a), wide, size))

    if aside:
        aside.tick(ticked + i + 2)

    @pl.when(step == steps - 1)
    def _():
        for n in range(4):
            g_out[:, n * full : (n + 1) * full] = g_s[n].astype(BF16)
        if aside:
            aside.run(steps * (steps + 2) - steps * (steps - 1) // 2)
            aside.drain()
            aside.hand_out(summed)


def att_back(layer, by, kept, w, more, sums=(), number=None):
    q, k, v, att, _, h, lse = kept
    layers, d, full = w["wq"].shape
    assert d == full
    tokens = by.shape[1]
    last = tokens // TILE - 1
    heads = full // HEAD
    whole = lambda shape: pl.BlockSpec(shape, lambda i: (0,) * len(shape))
    one = lambda shape: pl.BlockSpec((1, *shape), lambda i: (layer, 0, 0), pipeline_mode=pl.Buffered(1))
    tile = lambda n: pl.BlockSpec((1, TILE, d), lambda i: (n, last - i, 0))
    tables = rotary_tables(tokens)
    operands, specs, out_specs, out_shapes, scratch, where = hosted(sums)
    return pl.pallas_call(
        functools.partial(att_back_kernel, more, where, tokens // TILE),
        grid=(tokens // TILE,),
        in_specs=[tile(0), tile(layer), tile(layer), one((tokens, full)), one((tokens, full)), tile(layer),
                  pl.BlockSpec((1, 8, TILE), lambda i: (layer, 0, last - i)), *(whole(t.shape) for t in tables),
                  one((d, full)), one((d, full)), one((d, full)), one((full, d)), *specs],
        out_specs=[tile(0)] * more + [pl.BlockSpec((d, 4 * full), lambda i: (0, 0), pipeline_mode=pl.Buffered(1)), *out_specs],
        out_shape=[jax.ShapeDtypeStruct((1, tokens, d), BF16)] * more + [jax.ShapeDtypeStruct((d, 4 * full), BF16), *out_shapes],
        scratch_shapes=[pltpu.VMEM((tokens, HALF), F32), pltpu.VMEM((tokens, HALF), F32), pltpu.VMEM((heads, HEAD, TILE), F32),
                        pltpu.VMEM((tokens, full), F32), pltpu.VMEM((tokens, full), F32), pltpu.VMEM((4, d, full), F32),
                        pltpu.VMEM((TILE, full), BF16), pltpu.VMEM((8, TILE), F32), *scratch],
        compiler_params=host_params(sums, number),
        cost_estimate=pl.CostEstimate(flops=2 * tokens * d * (8 * d + 3 * tokens), bytes_accessed=20 * tokens * d, transcendentals=tokens * tokens * heads // 2),
        name="att_back",
    )(by, h, q, k, v, att, lse, *tables, w["wq"], w["wk"], w["wv"], w["wo"], *operands)


BESIDE = {("mlp", 1): 0, ("att", 1): 7, ("mlp", 0): 9, ("att", 0): 7}


def units_of(names, m_shapes):
    out = []
    for name in names:
        _, rows, width = m_shapes[name]
        out += [(name, r, c) for r in range(0, rows, ROWS) for c in range(0, width, UNIT)]
    return out


def finish_kernel(places, units, ready, shapes, count, *refs):
    refs = list(refs)
    take = lambda n: [refs.pop(0) for _ in range(n)]
    raw, done = take(1 + max(n for n, _ in places)), take(len(ready))
    w, m, v = (dict(zip(NAMES, take(7))) for _ in range(3))
    new = dict(zip(NAMES, take(7)))
    g_out, factor_out = take(2)
    ws, ns, ms, vs = (dict(zip(NAMES, take(7))) for _ in range(4))
    last = Sum(raw, places, take(8))
    (g_s, part, parts, factor_s, done_sem, load_sem, store_sem, nsend, nrecv, asend, arecv) = refs
    me, z, core, partner, left, right = last.me, last.z, last.core, last.partner, last.left, last.right
    total, layers = last.total, shapes["wq"][0]

    loads = [pltpu.make_async_copy(ref, g_s.at[pl.ds(at, ref.shape[0])], done_sem.at[n]) for n, (ref, at) in enumerate(zip(done, ready))]
    for i, name in enumerate(NAMES):
        rows = shapes[name][1]
        loads.append(pltpu.make_async_copy(w[name].at[:, pl.ds(pl.multiple_of(me * rows, ROWS), rows), :], ws[name], load_sem.at[0, i]))
        loads.append(pltpu.make_async_copy(m[name], ms[name], load_sem.at[1, i]))
        loads.append(pltpu.make_async_copy(v[name], vs[name], load_sem.at[2, i]))
    last.start()
    for c in loads:
        c.start()
    last.run(0)
    last.drain()
    for c in loads:
        c.wait()
    for n in range(total):
        g_s[n] = last.own[n, z]

    def squares(n, sofar):
        g = g_s[n].astype(F32)
        return sofar + g * g

    size = lax.fori_loop(0, len(units), squares, jnp.zeros((ROWS, UNIT), F32))
    part[...] = jnp.broadcast_to(jnp.sum(size, keepdims=True), part.shape)
    parts[me] = part[...]
    tell = [to(part, parts.at[me], nsend.at[o], nrecv.at[o], lax.rem(me + o, 8)) for o in range(1, 8)]
    for c in tell:
        c.start()
    for c in tell:
        c.wait_recv()
    size = parts[0]
    for o in range(1, 8):
        size = size + parts[o]
    factor_s[...] = jnp.minimum(1.0, 0.5 * lax.rsqrt(size / count + 1e-30))
    factor = factor_s[:1, :1]

    pieces = [(name, layer) for layer in reversed(range(layers)) for name in MLP] + [(name, layer) for layer in reversed(range(layers)) for name in ATT]

    def region(ref, name, layer, chip, c):
        rows = shapes[name][1]
        return ref[name].at[layer, pl.ds(pl.multiple_of((2 * chip + c) * rows, ROWS), rows), :]

    def share(p, slot, chip, first, who, core_of):
        name, layer = pieces[p]
        there = region(new, name, layer, chip, core_of)
        src = ns[name].at[layer] if first else there
        return to(src, there, asend.at[slot, p], arecv.at[slot, p], who)

    stores = [pltpu.make_async_copy(g_s, g_out, store_sem.at[len(pieces)]), pltpu.make_async_copy(factor_s, factor_out, store_sem.at[len(pieces) + 1])]
    for p in range(len(pieces) + 3):
        if p < len(pieces):
            name, layer = pieces[p]
            for u, (uname, ulayer, r, c) in enumerate(units):
                if (uname, ulayer) != (name, layer):
                    continue
                at = (layer, slice(r, r + ROWS), slice(c, c + UNIT))
                ns[name][at] = adamw(ws[name][at].astype(F32), ms[name][at], vs[name][at], g_s[u].astype(F32) * factor)[0]

            @pl.when(z < 3)
            def _():
                share(p, 1, z, True, right, core).start()

            @pl.when(z > 0)
            def _():
                share(p, 4, z, True, left, core).start()

            share(p, 0, z, True, partner, core).start()
            stores.append(pltpu.make_async_copy(ns[name].at[layer], region(new, name, layer, z, core), store_sem.at[p]))
            stores[-1].start()
            if p == 0:
                for c in stores[:2]:
                    c.start()
        for far in (1, 2, 3):
            q = p - far
            if not 0 <= q < len(pieces):
                continue

            @pl.when(z >= far)
            def _():
                share(q, far, z - far, False, right, core).wait_recv()
                if far < 3:
                    @pl.when(z < 3)
                    def _():
                        share(q, far + 1, z - far, False, right, core).start()
                share(q, 6 + far, z - far, False, partner, core).start()

            @pl.when(z <= 3 - far)
            def _():
                share(q, 3 + far, z + far, False, left, core).wait_recv()
                if far < 3:
                    @pl.when(z > 0)
                    def _():
                        share(q, 4 + far, z + far, False, left, core).start()
                share(q, 9 + far, z + far, False, partner, core).start()

    for c in tell:
        c.wait_send()
    for p in range(len(pieces)):
        mine, theirs = share(p, 0, z, True, partner, core), share(p, 0, z, False, partner, 1 - core)
        mine.wait_send()
        theirs.wait_recv()

        @pl.when(z < 3)
        def _():
            share(p, 1, z, True, right, core).wait_send()

        @pl.when(z > 0)
        def _():
            share(p, 4, z, True, left, core).wait_send()

        for far in (1, 2, 3):
            @pl.when(z >= far)
            def _():
                if far < 3:
                    @pl.when(z < 3)
                    def _():
                        share(p, far + 1, z - far, False, right, core).wait_send()
                share(p, 6 + far, z - far, False, partner, core).wait_send()
                share(p, 6 + far, z - far, False, partner, 1 - core).wait_recv()

            @pl.when(z <= 3 - far)
            def _():
                if far < 3:
                    @pl.when(z > 0)
                    def _():
                        share(p, 4 + far, z + far, False, left, core).wait_send()
                share(p, 9 + far, z + far, False, partner, core).wait_send()
                share(p, 9 + far, z + far, False, partner, 1 - core).wait_recv()
    for c in stores:
        c.wait()


def adamw(w, m, v, g):
    m = 0.9 * m + 0.1 * g
    v = 0.95 * v + 0.05 * g * g
    return (w - 0.02 * (m * lax.rsqrt(v + 1e-8) + 0.1 * w)).astype(BF16), m, v


def moments_kernel(units, g_ref, factor_ref, *refs):
    m, v, m_out, v_out = (dict(zip(NAMES, refs[i : i + 7])) for i in range(0, 28, 7))
    layer = pl.program_id(0)
    factor = factor_ref[:1, :1]

    for which in sorted({u[1] for u in units}):
        @pl.when(layer == which)
        def _():
            for n, (name, one, r, c) in enumerate(units):
                if one == which:
                    at = (0, slice(r, r + ROWS), slice(c, c + UNIT))
                    _, m_out[name][at], v_out[name][at] = adamw(0.0, m[name][at], v[name][at], g_ref[n].astype(F32) * factor)


def moments(units, g, factor, m, v):
    specs = [pl.BlockSpec((1, *one.shape[1:]), lambda l: (l, 0, 0)) for one in (*m, *v)]
    whole = lambda a: pl.BlockSpec(a.shape, lambda l: (0,) * a.ndim)
    return pl.pallas_call(
        functools.partial(moments_kernel, units),
        grid=(m[0].shape[0],),
        in_specs=[whole(g), whole(factor), *specs],
        out_specs=specs,
        out_shape=[jax.ShapeDtypeStruct(one.shape, F32) for one in (*m, *v)],
        compiler_params=pltpu.CompilerParams(dimension_semantics=("arbitrary",), vmem_limit_bytes=VMEM),
        cost_estimate=pl.CostEstimate(flops=10**7, bytes_accessed=2 * 10**7, transcendentals=0),
        name="moments",
    )(g, factor, *m, *v)


def finish(raw, ready, weights, m, v):
    shapes = {name: one.shape for name, one in zip(NAMES, m, strict=True)}
    operands, _, _, _, scratch, places = hosted([(g, at) for g, at, _ in raw])
    units, first = [u for _, _, u in raw], []
    for _, more in ready:
        first.append(len(units))
        units += more
    count = 8 * sum(one.size for one in m)
    any_ = pl.BlockSpec(memory_space=pl.ANY)
    pieces = 7 * m[0].shape[0]
    vmem = lambda dtype: [pltpu.VMEM(one.shape, dtype) for one in m]
    operands = operands + [g for g, _ in ready] + [*weights, *m, *v]
    g_shape, factor_shape = (len(units), ROWS, UNIT), (8, 128)
    *new, g, factor = pl.pallas_call(
        functools.partial(finish_kernel, places, units, first, shapes, count),
        in_specs=[any_] * len(operands),
        out_specs=[any_] * 9,
        out_shape=[jax.ShapeDtypeStruct(one.shape, BF16) for one in weights]
        + [jax.ShapeDtypeStruct(g_shape, BF16), jax.ShapeDtypeStruct(factor_shape, F32)],
        scratch_shapes=vmem(BF16) + vmem(BF16) + vmem(F32) + vmem(F32) + scratch + [
            pltpu.VMEM(g_shape, BF16), pltpu.VMEM((8, 128), F32), pltpu.VMEM((8, 8, 128), F32), pltpu.VMEM(factor_shape, F32),
            DMA((max(len(ready), 1),)), DMA((3, 7)), DMA((pieces + 2,)), DMA((8,)), DMA((8,)), DMA((13, pieces)), DMA((13, pieces))],
        compiler_params=pltpu.CompilerParams(collective_id=0, has_side_effects=True, vmem_limit_bytes=VMEM),
        cost_estimate=pl.CostEstimate(flops=10**9, bytes_accessed=10**8, transcendentals=0),
        name="finish",
    )(*operands)
    return (*new, *moments(units, g, factor, m, v))


def solution(mesh):
    def step(x, dy, *arrays):
        weights, m, v = (arrays[i : i + 7] for i in (0, 7, 14))
        w = dict(zip(NAMES, weights, strict=True))
        layers, d, _ = w["w_gate"].shape
        assert d == ROWS * lax.axis_size("dp") and lax.axis_size("dp") == 8
        shapes = {name: one.shape for name, one in zip(NAMES, m, strict=True)}
        kept = forward(x, w)
        by, waiting, ready = dy, [], []
        offer = lambda g, layer, names: [(g, n * UNIT, (name, layer, r, c)) for n, (name, r, c) in enumerate(units_of(names, shapes))]
        for n in reversed(range(layers)):
            now, waiting = waiting[: BESIDE["mlp", n]], waiting[BESIDE["mlp", n] :]
            by_h1, mlp, *summed = mlp_back(n, n, by, kept[4], w, [t[:2] for t in now], 2 * n + 1)
            ready += [(one, [t[2] for t in now]) for one in summed]
            waiting += offer(mlp, n, MLP)
            now, waiting = waiting[: BESIDE["att", n]], waiting[BESIDE["att", n] :]
            *by_h, att = out = att_back(n, by_h1, kept, w, n > 0, [t[:2] for t in now], 2 * n + 2)
            if now:
                *by_h, att, summed = out
                ready.append((summed, [t[2] for t in now]))
            waiting += offer(att, n, ATT)
            by = by_h[0] if by_h else None
        return tuple(finish(waiting, ready, weights, m, v))

    states, all_of, cut = P(("rep", "dp"), None, None), P(None, None, None), P(None, "dp", None)
    return jax.shard_map(
        step,
        mesh=mesh,
        in_specs=(states, states) + (all_of,) * 7 + (cut,) * 14,
        out_specs=(P("rep", None, None),) * 7 + (P("rep", "dp", None),) * 14,
        check_vma=False,
    )
```

```python
import functools

import jax
import jax.numpy as jnp
import numpy as np
from jax import lax
from jax.experimental import pallas as pl
from jax.experimental.pallas import tpu as pltpu
from jax.sharding import PartitionSpec as P

NEG = -1e30
HIDDEN = 2 * NEG
LOG2E = 1.4426950408889634
VMEM = 60 * 2**20
HEAD = 256
HALF = 128
THETA = 10000
TILE = 512
PART = 512
FINE = 64
NAMES = ("wq", "wk", "wv", "wo", "w_gate", "w_up", "w_down")
F32, BF16 = jnp.float32, jnp.bfloat16


def dot(a, b, ca=1, cb=0):
    return lax.dot_general(a, b, (((ca,), (cb,)), ((), ())), preferred_element_type=F32)


def dot_t(a, b):
    return dot(a, b, 1, 1)


def rotary_tables(tokens):
    rate = float(THETA) ** (-np.arange(HALF, dtype=np.float64) / HALF)
    coarse = np.arange(0, tokens, FINE, dtype=np.float64)[:, None] * rate
    fine = np.arange(FINE, dtype=np.float64)[:, None] * rate
    return [jnp.asarray(f(t), F32) for t in (coarse, fine) for f in (np.cos, np.sin)]


def fill_rotary(tables, cos_s, sin_s):
    ca, sa, cb, sb = (t[...] for t in tables)
    for n in range(ca.shape[0]):
        c, s = ca[n : n + 1, :], sa[n : n + 1, :]
        cos_s[n * FINE : (n + 1) * FINE, :] = c * cb - s * sb
        sin_s[n * FINE : (n + 1) * FINE, :] = s * cb + c * sb


def turn(t, cos, sin):
    out = []
    for at in range(0, t.shape[1], HEAD):
        a, b = t[:, at : at + HALF], t[:, at + HALF : at + HEAD]
        out += [a * cos - b * sin, b * cos + a * sin]
    return jnp.concatenate(out, axis=1)


def norm_of(wide):
    scale = lax.rsqrt(jnp.mean(wide * wide, -1, keepdims=True) + 1e-6)
    return (wide * scale).astype(BF16), scale


def norm_back(by, wide, scale):
    along = jnp.sum(by * wide, -1, keepdims=True) * (1 / wide.shape[1])
    return (scale * by - wide * (scale * scale * scale * along)).astype(BF16)


def rounded(t):
    return t.astype(BF16).astype(F32)


def add(a, b):
    return (a.astype(F32) + b.astype(F32)).astype(BF16)


def diagonal():
    return lax.broadcasted_iota(jnp.int32, (TILE, TILE), 1) >= lax.broadcasted_iota(jnp.int32, (TILE, TILE), 0)


LAG = 2
MESH = pl.DeviceIdType.MESH
UNIT = 512
ROWS = 64
ATT, MLP = NAMES[:4], NAMES[4:]
DMA = pltpu.SemaphoreType.DMA


def to(src, dst, s_sem, r_sem, who):
    return pltpu.make_async_remote_copy(src_ref=src, dst_ref=dst, send_sem=s_sem, recv_sem=r_sem, device_id={"dp": who}, device_id_type=MESH)


def meet(me):
    barrier = pltpu.get_barrier_semaphore()
    for o in range(1, 8):
        pl.semaphore_signal(barrier, inc=1, device_id={"dp": lax.rem(me + o, 8)}, device_id_type=MESH)
    pl.semaphore_wait(barrier, 7)


def sum_scratch(total):
    return [pltpu.VMEM((total, 4, ROWS, UNIT), BF16), pltpu.VMEM((total, 4, ROWS, UNIT), BF16), pltpu.VMEM((total, 5, ROWS, UNIT), BF16),
            DMA((total,)), DMA((total,)), DMA((total,)), DMA((total, 4)), DMA((total, 5))]


class Sum:
    def __init__(self, raw, where, scratch):
        self.raw, self.where, self.total = raw, where, len(where)
        self.ticks = self.total + 3 * LAG
        self.own, self.other, self.came, self.own_sem, self.psend, self.precv, self.send, self.recv = scratch
        self.me = lax.axis_index("dp")
        self.z, self.core = lax.div(self.me, 2), lax.rem(self.me, 2)
        self.partner = 2 * self.z + 1 - self.core
        self.left, self.right = jnp.maximum(self.me - 2, 0), jnp.minimum(self.me + 2, 7)

    def swap(self, n):
        k, at = self.where[n]
        return to(self.raw[k].at[:, 1 - self.core, :, pl.ds(at, UNIT)], self.other.at[n], self.psend.at[n], self.precv.at[n], self.partner)

    def start(self):
        for n, (k, at) in enumerate(self.where):
            pltpu.make_async_copy(self.raw[k].at[:, self.core, :, pl.ds(at, UNIT)], self.own.at[n], self.own_sem.at[n]).start()
        meet(self.me)
        for n in range(self.total):
            self.swap(n).start()

    def both(self, c, t):
        return self.own[c, t].astype(F32) + self.other[c, t].astype(F32)

    def hop(self, c, t, slot, who):
        return to(self.own.at[c, t], self.came.at[c, slot], self.send.at[c, t], self.recv.at[c, slot], who)

    def pass_on(self, c, t, first, slot, who):
        @pl.when(first)
        def _():
            self.own[c, t] = self.both(c, t).astype(BF16)

        @pl.when(jnp.logical_not(first))
        def _():
            self.hop(c, t, t, who).wait_recv()
            self.own[c, t] = (self.both(c, t) + self.came[c, t].astype(F32)).astype(BF16)

        self.hop(c, t, slot, who).start()

    def tick(self, t):
        total, z = self.total, self.z

        @pl.when(t < total)
        def _():
            pltpu.make_async_copy(self.own.at[t], self.own.at[t], self.own_sem.at[t]).wait()
            to(self.own.at[t], self.other.at[t], self.psend.at[t], self.precv.at[t], self.partner).wait_recv()

        c = t - LAG * z

        @pl.when((c >= 0) & (c < total))
        def _():
            for b in (3, 2, 1):
                @pl.when(z < b)
                def _():
                    self.pass_on(c, b, z == 0, b, self.right)

        d = t - LAG * (3 - z)

        @pl.when((d >= 0) & (d < total))
        def _():
            for b in (0, 1, 2):
                @pl.when(z > b)
                def _():
                    self.pass_on(d, b, z == 3, jnp.where(z == b + 1, 4, b), self.left)

        f = t - 3 * LAG

        @pl.when((f >= 0) & (f < total))
        def _():
            @pl.when(z > 0)
            def _():
                self.hop(f, z, z, self.right).wait_recv()

            @pl.when(z < 3)
            def _():
                self.hop(f, z, 4, self.left).wait_recv()

            mine = self.both(f, z)

            @pl.when(z == 0)
            def _():
                self.own[f, z] = (mine + self.came[f, 4].astype(F32)).astype(BF16)

            @pl.when(z == 3)
            def _():
                self.own[f, z] = (mine + self.came[f, z].astype(F32)).astype(BF16)

            @pl.when((z > 0) & (z < 3))
            def _():
                self.own[f, z] = (mine + self.came[f, z].astype(F32) + self.came[f, 4].astype(F32)).astype(BF16)

    def run(self, first):
        lax.fori_loop(first, self.ticks, lambda t, _: self.tick(t), None)

    def drain(self):
        def one(c, _):
            to(self.own.at[c], self.other.at[c], self.psend.at[c], self.precv.at[c], self.partner).wait_send()
            for b in range(4):
                @pl.when(self.z != b)
                def _():
                    self.hop(c, b, b, self.right).wait_send()

        lax.fori_loop(0, self.total, one, None)

    def hand_out(self, out):
        c = pltpu.make_async_copy(self.own.at[:, self.z], out, self.own_sem.at[0])
        c.start()
        c.wait()


def forward_kernel(x_ref, ca, sa, cb, sb, wq, wk, wv, wo, wg, wu, wd, q_out, k_out, v_out, att_out, h1_out, h_out, lse_out,
                   cos_s, sin_s, h_s, k_s, vt_s, top_s, mix_s):
    layer, i = pl.program_id(0), pl.program_id(1)
    heads = wq.shape[2] // HEAD
    e = HEAD**-0.5 * LOG2E
    here = pl.ds(pl.multiple_of(i * TILE, TILE), TILE)

    @pl.when((layer == 0) & (i == 0))
    def _():
        fill_rotary((ca, sa, cb, sb), cos_s, sin_s)
        vt_s[...] = jnp.ones_like(vt_s)

    @pl.when(layer == 0)
    def _():
        h_s[here, :] = x_ref[0]

    h = h_s[here, :]
    h_out[0] = h
    a, _ = norm_of(h.astype(F32))
    cos, sin = cos_s[here, :], sin_s[here, :]
    q = turn(rounded(dot(a, wq[0])), cos, sin).astype(BF16)
    k = turn(rounded(dot(a, wk[0])), cos, sin).astype(BF16)
    v = dot(a, wv[0]).astype(BF16)
    q_out[0], k_out[0], v_out[0] = q, k, v
    k_s[here, :] = k
    vt = v.T
    for n in range(heads):
        vt_s[n, :HEAD, here] = vt[n * HEAD : (n + 1) * HEAD, :]

    top_s[...] = jnp.full_like(top_s, NEG)
    mix_s[...] = jnp.zeros_like(mix_s)

    def block(j, masked):
        at = pl.ds(pl.multiple_of(j * TILE, TILE), TILE)
        qq = q_out[0]
        scores = [dot_t(k_s[at, n * HEAD : (n + 1) * HEAD], qq[:, n * HEAD : (n + 1) * HEAD]) for n in range(heads)]
        weights, keeps = [], []
        for n, s in enumerate(scores):
            if masked:
                s = jnp.where(diagonal(), s, HIDDEN)
            old = top_s[n : n + 1, :]
            top = jnp.maximum(old, s.max(axis=0, keepdims=True))
            top_s[n : n + 1, :] = top
            weights.append(jnp.exp2((s - top) * e).astype(BF16))
            keeps.append(jnp.exp2((old - top) * e))
        for n in range(heads):
            mix_s[n] = mix_s[n] * keeps[n] + dot(vt_s[n, :, at], weights[n])

    lax.fori_loop(0, i, lambda j, _: block(j, False), None)
    block(i, True)
    out = []
    for n in range(heads):
        total = mix_s[n, HEAD : HEAD + 1, :]
        out.append((mix_s[n, :HEAD, :] * (1 / total)).T.astype(BF16))
        lse_out[0, n : n + 1, :] = top_s[n : n + 1, :] * e + jnp.log2(total)
    att = jnp.concatenate(out, axis=1)
    att_out[0] = att
    h1 = add(h, dot(att, wo[0]).astype(BF16))
    h1_out[0] = h1

    @pl.when(layer < pl.num_programs(0) - 1)
    def _():
        b, _ = norm_of(h1_out[0].astype(F32))
        total = None
        for at in range(0, wg.shape[2], PART):
            gate, up = dot(b, wg[0, :, at : at + PART]), dot(b, wu[0, :, at : at + PART])
            part = dot((gate * jax.nn.sigmoid(gate) * up).astype(BF16), wd[0, at : at + PART, :])
            total = part if total is None else total + part
        h_s[here, :] = add(h1_out[0], total.astype(BF16))


def forward(x, w):
    layers, d, wide = w["wq"].shape
    tokens, hidden = x.shape[1], w["w_gate"].shape[2]
    assert tokens % TILE == 0 and hidden % PART == 0
    heads = wide // HEAD
    whole = lambda shape: pl.BlockSpec(shape, lambda l, i: (0,) * len(shape))
    each = lambda shape: pl.BlockSpec((1, *shape), lambda l, i: (l, 0, 0))
    most = lambda shape: pl.BlockSpec((1, *shape), lambda l, i: (jnp.minimum(l, layers - 2), 0, 0))
    tile = lambda width: pl.BlockSpec((1, TILE, width), lambda l, i: (l, i, 0))
    tables = rotary_tables(tokens)
    flops = 2 * tokens * (layers * d * wide * 4 + (layers - 1) * 3 * d * hidden + layers * tokens * wide)
    return pl.pallas_call(
        forward_kernel,
        grid=(layers, tokens // TILE),
        in_specs=[pl.BlockSpec((1, TILE, d), lambda l, i: (0, jnp.where(l == 0, i, tokens // TILE - 1), 0)), *(whole(t.shape) for t in tables),
                  each((d, wide)), each((d, wide)), each((d, wide)), each((wide, d)), most((d, hidden)), most((d, hidden)), most((hidden, d))],
        out_specs=[tile(wide)] * 4 + [tile(d)] * 2 + [pl.BlockSpec((1, 8, TILE), lambda l, i: (l, 0, i))],
        out_shape=[jax.ShapeDtypeStruct((layers, tokens, wide), BF16)] * 4 + [jax.ShapeDtypeStruct((layers, tokens, d), BF16)] * 2
        + [jax.ShapeDtypeStruct((layers, 8, tokens), F32)],
        scratch_shapes=[pltpu.VMEM((tokens, HALF), F32), pltpu.VMEM((tokens, HALF), F32), pltpu.VMEM((tokens, d), BF16),
                        pltpu.VMEM((tokens, wide), BF16), pltpu.VMEM((heads, HEAD + 16, tokens), BF16), pltpu.VMEM((8, TILE), F32),
                        pltpu.VMEM((heads, HEAD + 16, TILE), F32)],
        compiler_params=pltpu.CompilerParams(dimension_semantics=("arbitrary", "arbitrary"), vmem_limit_bytes=VMEM),
        cost_estimate=pl.CostEstimate(flops=flops, bytes_accessed=40 * tokens * d, transcendentals=tokens * tokens * heads),
        name="forward",
    )(x, *tables, *(w[n] for n in NAMES))


def mlp_back_kernel(by_ref, h1_ref, wg, wu, wd, by_h1, g_out, dg_s, du_s, dd_s):
    i = pl.program_id(0)
    hidden = wg.shape[2]

    @pl.when(i == 0)
    def _():
        for s in (dg_s, du_s, dd_s):
            s[...] = jnp.zeros_like(s)

    by, wide = by_ref[0], h1_ref[0].astype(F32)
    b, scale = norm_of(wide)
    bt, byt = b.T, by.T
    by_b = [None, None]
    for at in range(0, hidden, PART):
        cut = slice(at, at + PART)
        gate, up = dot(b, wg[0, :, cut]), dot(b, wu[0, :, cut])
        by_p = rounded(dot_t(by, wd[0, cut, :]))
        s = jax.nn.sigmoid(gate)
        act = gate * s
        p = (act * up).astype(BF16)
        by_up = (by_p * act).astype(BF16)
        by_gate = (by_p * up * (s + act * (1 - s))).astype(BF16)
        dd_s[:, cut] += dot(byt, p)
        dg_s[:, cut] += dot(bt, by_gate)
        du_s[:, cut] += dot(bt, by_up)
        parts = dot_t(by_gate, wg[0, :, cut]), dot_t(by_up, wu[0, :, cut])
        by_b = [new if old is None else old + new for old, new in zip(by_b, parts)]
    by_h1[0] = add(by, norm_back(rounded(rounded(by_b[0]) + rounded(by_b[1])), wide, scale))

    @pl.when(i == pl.num_programs(0) - 1)
    def _():
        g_out[:, :hidden] = dg_s[...].astype(BF16)
        g_out[:, hidden : 2 * hidden] = du_s[...].astype(BF16)
        d = by.shape[1]
        ways = d // ROWS
        deep = hidden // ways
        for n in range(ways):
            own = dd_s[:, n * deep : (n + 1) * deep].T.astype(BF16)
            for c in range(deep // ROWS):
                g_out[n * ROWS : (n + 1) * ROWS, 2 * hidden + c * d : 2 * hidden + (c + 1) * d] = own[c * ROWS : (c + 1) * ROWS, :]


def mlp_back(layer, at, by, h1, w):
    layers, d, hidden = w["w_gate"].shape
    tokens = by.shape[1]
    one = lambda shape: pl.BlockSpec((1, *shape), lambda i: (layer, 0, 0), pipeline_mode=pl.Buffered(1))
    tile = lambda n: pl.BlockSpec((1, TILE, d), lambda i: (n, i, 0))
    return pl.pallas_call(
        mlp_back_kernel,
        grid=(tokens // TILE,),
        in_specs=[tile(0), tile(at), one((d, hidden)), one((d, hidden)), one((hidden, d))],
        out_specs=[tile(0), pl.BlockSpec((d, 3 * hidden), lambda i: (0, 0), pipeline_mode=pl.Buffered(1))],
        out_shape=[jax.ShapeDtypeStruct((1, tokens, d), BF16), jax.ShapeDtypeStruct((d, 3 * hidden), BF16)],
        scratch_shapes=[pltpu.VMEM((d, hidden), F32)] * 3,
        compiler_params=pltpu.CompilerParams(dimension_semantics=("arbitrary",), vmem_limit_bytes=VMEM),
        cost_estimate=pl.CostEstimate(flops=16 * tokens * d * hidden, bytes_accessed=20 * tokens * d, transcendentals=tokens * hidden),
        name="mlp_back",
    )(by, h1, w["w_gate"], w["w_up"], w["w_down"])


def att_back_kernel(more, by_ref, h_ref, q_ref, k_ref, v_ref, att_ref, lse_ref, ca, sa, cb, sb, wq, wk, wv, wo, *rest):
    by_h, rest = (rest[0], rest[1:]) if more else (None, rest)
    g_out, cos_s, sin_s, dq_s, dk_s, dv_s, g_s, do_s, delta_s = rest
    step = pl.program_id(0)
    i = pl.num_programs(0) - 1 - step
    d, full = wq.shape[1], wq.shape[2]
    heads = full // HEAD
    scale = HEAD**-0.5
    e = scale * LOG2E
    here = pl.ds(pl.multiple_of(i * TILE, TILE), TILE)

    @pl.when(step == 0)
    def _():
        fill_rotary((ca, sa, cb, sb), cos_s, sin_s)
        for s in (dk_s, dv_s, g_s):
            s[...] = jnp.zeros_like(s)

    by = by_ref[0]
    by_att = dot_t(by, wo[0]).astype(BF16)
    do_s[...] = by_att
    att = att_ref[0]
    g_s[3] += dot(att.T, by)
    rows = by_att.astype(F32) * att.astype(F32)
    for n in range(heads):
        delta_s[n : n + 1, :] = rows[:, n * HEAD : (n + 1) * HEAD].T.sum(axis=0, keepdims=True)
    dq_s[...] = jnp.zeros_like(dq_s)

    def block(j, masked):
        at = pl.ds(pl.multiple_of(j * TILE, TILE), TILE)
        cuts = [slice(n * HEAD, (n + 1) * HEAD) for n in range(heads)]
        qs = [q_ref[0, :, c] for c in cuts]
        dos = [do_s[:, c] for c in cuts]
        scores = [dot_t(k_ref[0, at, c], qs[n]) for n, c in enumerate(cuts)]
        dps = [dot_t(v_ref[0, at, c], dos[n]) for n, c in enumerate(cuts)]
        for n, c in enumerate(cuts):
            p = jnp.exp2(scores[n] * e - lse_ref[0, n : n + 1, :])
            if masked:
                p = jnp.where(diagonal(), p, 0.0)
            ds = (p * (dps[n] - delta_s[n : n + 1, :])).astype(BF16)
            dv_s[at, c] += dot(p.astype(BF16), dos[n])
            dk_s[at, c] += dot(ds, qs[n])
            dq_s[n] += dot(k_ref[0, at, c].T, ds)

    lax.fori_loop(0, i, lambda j, _: block(j, False), None)
    block(i, True)

    cos, sin = cos_s[here, :], -sin_s[here, :]
    dq = jnp.concatenate([(dq_s[n] * scale).T for n in range(heads)], axis=1)
    dq = turn(rounded(dq), cos, sin).astype(BF16)
    dk = turn(rounded(dk_s[here, :] * scale), cos, sin).astype(BF16)
    dv = dv_s[here, :].astype(BF16)
    wide = h_ref[0].astype(F32)
    a, size = norm_of(wide)
    at = a.T
    for n, t in enumerate((dq, dk, dv)):
        g_s[n] += dot(at, t)
    if more:
        by_a = sum(rounded(dot_t(t, m[0])) for t, m in ((dq, wq), (dk, wk), (dv, wv)))
        by_h[0] = add(by, norm_back(rounded(by_a), wide, size))

    @pl.when(step == pl.num_programs(0) - 1)
    def _():
        for n in range(4):
            g_out[:, n * full : (n + 1) * full] = g_s[n].astype(BF16)


def att_back(layer, by, kept, w, more):
    q, k, v, att, _, h, lse = kept
    layers, d, full = w["wq"].shape
    assert d == full
    tokens = by.shape[1]
    last = tokens // TILE - 1
    heads = full // HEAD
    whole = lambda shape: pl.BlockSpec(shape, lambda i: (0,) * len(shape))
    one = lambda shape: pl.BlockSpec((1, *shape), lambda i: (layer, 0, 0), pipeline_mode=pl.Buffered(1))
    tile = lambda n: pl.BlockSpec((1, TILE, d), lambda i: (n, last - i, 0))
    tables = rotary_tables(tokens)
    return pl.pallas_call(
        functools.partial(att_back_kernel, more),
        grid=(tokens // TILE,),
        in_specs=[tile(0), tile(layer), tile(layer), one((tokens, full)), one((tokens, full)), tile(layer),
                  pl.BlockSpec((1, 8, TILE), lambda i: (layer, 0, last - i)), *(whole(t.shape) for t in tables),
                  one((d, full)), one((d, full)), one((d, full)), one((full, d))],
        out_specs=[tile(0)] * more + [pl.BlockSpec((d, 4 * full), lambda i: (0, 0), pipeline_mode=pl.Buffered(1))],
        out_shape=[jax.ShapeDtypeStruct((1, tokens, d), BF16)] * more + [jax.ShapeDtypeStruct((d, 4 * full), BF16)],
        scratch_shapes=[pltpu.VMEM((tokens, HALF), F32), pltpu.VMEM((tokens, HALF), F32), pltpu.VMEM((heads, HEAD, TILE), F32),
                        pltpu.VMEM((tokens, full), F32), pltpu.VMEM((tokens, full), F32), pltpu.VMEM((4, d, full), F32),
                        pltpu.VMEM((TILE, full), BF16), pltpu.VMEM((8, TILE), F32)],
        compiler_params=pltpu.CompilerParams(dimension_semantics=("arbitrary",), vmem_limit_bytes=VMEM),
        cost_estimate=pl.CostEstimate(flops=2 * tokens * d * (8 * d + 3 * tokens), bytes_accessed=20 * tokens * d, transcendentals=tokens * tokens * heads // 2),
        name="att_back",
    )(by, h, q, k, v, att, lse, *tables, w["wq"], w["wk"], w["wv"], w["wo"])


def sum_kernel(where, *refs):
    refs = list(refs)
    raw = [refs.pop(0) for _ in range(1 + max(n for n, _ in where))]
    out = refs.pop(0)
    work = Sum(raw, where, refs)
    work.start()
    work.run(0)
    work.drain()
    work.hand_out(out)


def summed(gradients):
    where = tuple((i, at) for i, g in enumerate(gradients) for at in range(0, g.shape[1], UNIT))
    operands = [g.reshape(4, 2, ROWS, -1) for g in gradients]
    any_ = pl.BlockSpec(memory_space=pl.ANY)
    return pl.pallas_call(
        functools.partial(sum_kernel, where),
        in_specs=[any_] * len(operands),
        out_specs=any_,
        out_shape=jax.ShapeDtypeStruct((len(where), ROWS, UNIT), BF16),
        scratch_shapes=sum_scratch(len(where)),
        compiler_params=pltpu.CompilerParams(collective_id=1, has_side_effects=True, vmem_limit_bytes=VMEM),
        cost_estimate=pl.CostEstimate(flops=5 * 10**10, bytes_accessed=10**7, transcendentals=0),
        name="summed",
    )(*operands)


def units_of(names, m_shapes):
    out = []
    for name in names:
        _, rows, width = m_shapes[name]
        out += [(name, r, c) for r in range(0, rows, ROWS) for c in range(0, width, UNIT)]
    return out


def finish_kernel(blocks, units, shapes, count, *refs):
    refs = list(refs)
    take = lambda n: [refs.pop(0) for _ in range(n)]
    done = take(len(blocks))
    w, m, v, new = (dict(zip(NAMES, take(7))) for _ in range(4))
    g_out, factor_out = take(2)
    ws, ns, ms, vs = (dict(zip(NAMES, take(7))) for _ in range(4))
    (g_s, part, parts, factor_s, done_sem, load_sem, store_sem, nsend, nrecv, asend, arecv) = refs
    me = lax.axis_index("dp")
    z, core = lax.div(me, 2), lax.rem(me, 2)
    partner = 2 * z + 1 - core
    left, right = jnp.maximum(me - 2, 0), jnp.minimum(me + 2, 7)
    layers = shapes["wq"][0]

    loads = []
    for ref, (start, n, at) in zip(done, blocks):
        if len(ref.shape) == 3:
            loads.append(pltpu.make_async_copy(ref.at[pl.ds(start, n)], g_s.at[pl.ds(at, n)], done_sem.at[at]))
        else:
            loads += [pltpu.make_async_copy(ref.at[:, pl.ds(start + i * UNIT, UNIT)], g_s.at[at + i], done_sem.at[at + i]) for i in range(n)]
    for i, name in enumerate(NAMES):
        rows = shapes[name][1]
        loads.append(pltpu.make_async_copy(w[name].at[:, pl.ds(pl.multiple_of(me * rows, ROWS), rows), :], ws[name], load_sem.at[0, i]))
        loads.append(pltpu.make_async_copy(m[name], ms[name], load_sem.at[1, i]))
        loads.append(pltpu.make_async_copy(v[name], vs[name], load_sem.at[2, i]))
    for c in loads:
        c.start()
    meet(me)
    for c in loads[: -3 * len(NAMES)]:
        c.wait()

    def squares(n, sofar):
        g = g_s[n].astype(F32)
        return sofar + g * g

    size = lax.fori_loop(0, len(units), squares, jnp.zeros((ROWS, UNIT), F32))
    part[...] = jnp.broadcast_to(jnp.sum(size, keepdims=True), part.shape)
    parts[me] = part[...]
    tell = [to(part, parts.at[me], nsend.at[o], nrecv.at[o], lax.rem(me + o, 8)) for o in range(1, 8)]
    for c in tell:
        c.start()
    for c in loads[-3 * len(NAMES) :]:
        c.wait()
    for c in tell:
        c.wait_recv()
    size = parts[0]
    for o in range(1, 8):
        size = size + parts[o]
    factor_s[...] = jnp.minimum(1.0, 0.5 * lax.rsqrt(size / count + 1e-30))
    factor = factor_s[:1, :1]

    pieces = [(name, layer) for names in (MLP, ATT) for layer in range(layers) for name in names]

    def region(ref, name, layer, chip, c):
        rows = shapes[name][1]
        return ref[name].at[layer, pl.ds(pl.multiple_of((2 * chip + c) * rows, ROWS), rows), :]

    def share(p, slot, chip, first, who, core_of):
        name, layer = pieces[p]
        there = region(new, name, layer, chip, core_of)
        src = ns[name].at[layer] if first else there
        return to(src, there, asend.at[slot, p], arecv.at[slot, p], who)

    stores = [pltpu.make_async_copy(g_s, g_out, store_sem.at[len(pieces)]), pltpu.make_async_copy(factor_s, factor_out, store_sem.at[len(pieces) + 1])]
    for p in range(len(pieces) + 3):
        if p < len(pieces):
            name, layer = pieces[p]
            for u, (uname, ulayer, r, c) in enumerate(units):
                if (uname, ulayer) != (name, layer):
                    continue
                at = (layer, slice(r, r + ROWS), slice(c, c + UNIT))
                ns[name][at] = adamw(ws[name][at].astype(F32), ms[name][at], vs[name][at], g_s[u].astype(F32) * factor)[0]

            @pl.when(z < 3)
            def _():
                share(p, 1, z, True, right, core).start()

            @pl.when(z > 0)
            def _():
                share(p, 4, z, True, left, core).start()

            share(p, 0, z, True, partner, core).start()
            stores.append(pltpu.make_async_copy(ns[name].at[layer], region(new, name, layer, z, core), store_sem.at[p]))
            stores[-1].start()
            if p == 0:
                for c in stores[:2]:
                    c.start()
        for far in (1, 2, 3):
            q = p - far
            if not 0 <= q < len(pieces):
                continue

            @pl.when(z >= far)
            def _():
                share(q, far, z - far, False, right, core).wait_recv()
                if far < 3:
                    @pl.when(z < 3)
                    def _():
                        share(q, far + 1, z - far, False, right, core).start()
                share(q, 6 + far, z - far, False, partner, core).start()

            @pl.when(z <= 3 - far)
            def _():
                share(q, 3 + far, z + far, False, left, core).wait_recv()
                if far < 3:
                    @pl.when(z > 0)
                    def _():
                        share(q, 4 + far, z + far, False, left, core).start()
                share(q, 9 + far, z + far, False, partner, core).start()

    for c in tell:
        c.wait_send()
    for p in range(len(pieces)):
        mine, theirs = share(p, 0, z, True, partner, core), share(p, 0, z, False, partner, 1 - core)
        mine.wait_send()
        theirs.wait_recv()

        @pl.when(z < 3)
        def _():
            share(p, 1, z, True, right, core).wait_send()

        @pl.when(z > 0)
        def _():
            share(p, 4, z, True, left, core).wait_send()

        for far in (1, 2, 3):
            @pl.when(z >= far)
            def _():
                if far < 3:
                    @pl.when(z < 3)
                    def _():
                        share(p, far + 1, z - far, False, right, core).wait_send()
                share(p, 6 + far, z - far, False, partner, core).wait_send()
                share(p, 6 + far, z - far, False, partner, 1 - core).wait_recv()

            @pl.when(z <= 3 - far)
            def _():
                if far < 3:
                    @pl.when(z > 0)
                    def _():
                        share(p, 4 + far, z + far, False, left, core).wait_send()
                share(p, 9 + far, z + far, False, partner, core).wait_send()
                share(p, 9 + far, z + far, False, partner, 1 - core).wait_recv()
    for c in stores:
        c.wait()


def adamw(w, m, v, g):
    m = 0.9 * m + 0.1 * g
    v = 0.95 * v + 0.05 * g * g
    return (w - 0.02 * (m * lax.rsqrt(v + 1e-8) + 0.1 * w)).astype(BF16), m, v


CUTS = 4


def results_kernel(units, g_ref, factor_ref, *refs):
    w, m, v, w_out, m_out, v_out = (dict(zip(NAMES, refs[i : i + 7])) for i in range(0, 42, 7))
    layer, cut = pl.program_id(0), pl.program_id(1)
    factor = factor_ref[:1, :1]
    for name in NAMES:
        w_out[name][...] = w[name][...]
    first = layer * len(units)

    for n, (name, r, c) in enumerate(units):
        rows = m[name].shape[1]
        here = (0, slice(0, rows), slice(c, c + UNIT))

        def do(g):
            _, m_out[name][here], v_out[name][here] = adamw(0.0, m[name][here], v[name][here], g.astype(F32) * factor)

        if rows == ROWS:
            @pl.when(cut == r // ROWS)
            def _():
                do(g_ref[first + n])
        else:
            do(g_ref[first + n, pl.ds(pl.multiple_of(cut * rows, rows), rows), :])


def results(units, g, factor, w, m, v):
    cut = lambda one: pl.BlockSpec((1, one.shape[1] // CUTS, one.shape[2]), lambda l, i: (l, i, 0))
    whole = lambda a: pl.BlockSpec(a.shape, lambda l, i: (0,) * a.ndim)
    arrays = (*w, *m, *v)
    return pl.pallas_call(
        functools.partial(results_kernel, units),
        grid=(m[0].shape[0], CUTS),
        in_specs=[whole(g), whole(factor), *(cut(a) for a in arrays)],
        out_specs=[cut(a) for a in arrays],
        out_shape=[jax.ShapeDtypeStruct(a.shape, a.dtype) for a in arrays],
        compiler_params=pltpu.CompilerParams(dimension_semantics=("arbitrary", "arbitrary"), vmem_limit_bytes=VMEM),
        cost_estimate=pl.CostEstimate(flops=10**7, bytes_accessed=5 * 10**7, transcendentals=0),
        name="results",
    )(g, factor, *arrays)


def finish(groups, weights, m, v):
    shapes = {name: one.shape for name, one in zip(NAMES, m, strict=True)}
    in_layer = units_of(NAMES, shapes)
    layers = m[0].shape[0]
    units = [(name, layer, r, c) for layer in range(layers) for name, r, c in in_layer]
    blocks = [(start, len(units_of(names, shapes)), units.index((names[0], layer, 0, 0))) for _, start, layer, names in groups]
    count = 8 * sum(one.size for one in m)
    any_ = pl.BlockSpec(memory_space=pl.ANY)
    pieces = 7 * layers
    vmem = lambda dtype: [pltpu.VMEM(one.shape, dtype) for one in m]
    operands = [g for g, *_ in groups] + [*weights, *m, *v]
    g_shape, factor_shape = (len(units), ROWS, UNIT), (8, 128)
    *new, g, factor = pl.pallas_call(
        functools.partial(finish_kernel, blocks, units, shapes, count),
        in_specs=[any_] * len(operands),
        out_specs=[any_] * 9,
        out_shape=[jax.ShapeDtypeStruct(one.shape, BF16) for one in weights]
        + [jax.ShapeDtypeStruct(g_shape, BF16), jax.ShapeDtypeStruct(factor_shape, F32)],
        scratch_shapes=vmem(BF16) + vmem(BF16) + vmem(F32) + vmem(F32) + [
            pltpu.VMEM(g_shape, BF16), pltpu.VMEM((8, 128), F32), pltpu.VMEM((8, 8, 128), F32), pltpu.VMEM(factor_shape, F32),
            DMA((len(units),)), DMA((3, 7)), DMA((pieces + 2,)), DMA((8,)), DMA((8,)), DMA((13, pieces)), DMA((13, pieces))],
        compiler_params=pltpu.CompilerParams(collective_id=2, has_side_effects=True, vmem_limit_bytes=VMEM),
        cost_estimate=pl.CostEstimate(flops=10**9, bytes_accessed=10**8, transcendentals=0),
        name="finish",
    )(*operands)
    return results(in_layer, g, factor, new, m, v)


def solution(mesh):
    def step(x, dy, *arrays):
        weights, m, v = (arrays[i : i + 7] for i in (0, 7, 14))
        w = dict(zip(NAMES, weights, strict=True))
        layers, d, _ = w["w_gate"].shape
        assert d == ROWS * lax.axis_size("dp") and lax.axis_size("dp") == 8
        kept = forward(x, w)
        by, groups, late = dy, [], []
        for n in reversed(range(layers)):
            by_h1, mlp = mlp_back(n, n, by, kept[4], w)
            groups.append((lax.psum_scatter(mlp, "dp", scatter_dimension=0, tiled=True), 0, n, MLP))
            *by_h, att = att_back(n, by_h1, kept, w, n > 0)
            late.append((att, n))
            by = by_h[0] if by_h else by
        blocks = summed([att for att, _ in late])
        groups += [(blocks, i * len(ATT), n, ATT) for i, (_, n) in enumerate(late)]
        return tuple(finish(groups, weights, m, v))

    states, all_of, cut = P(("rep", "dp"), None, None), P(None, None, None), P(None, "dp", None)
    return jax.shard_map(
        step,
        mesh=mesh,
        in_specs=(states, states) + (all_of,) * 7 + (cut,) * 14,
        out_specs=(P("rep", None, None),) * 7 + (P("rep", "dp", None),) * 14,
        check_vma=False,
    )
```

```python
import functools

import jax
import jax.numpy as jnp
import numpy as np
from jax import lax
from jax.experimental import pallas as pl
from jax.experimental.pallas import tpu as pltpu
from jax.sharding import PartitionSpec as P

NEG = -1e30
HIDDEN = 2 * NEG
LOG2E = 1.4426950408889634
VMEM = 60 * 2**20
HEAD = 256
HALF = 128
THETA = 10000
TILE = 512
PART = 512
FINE = 64
NAMES = ("wq", "wk", "wv", "wo", "w_gate", "w_up", "w_down")
F32, BF16 = jnp.float32, jnp.bfloat16


def dot(a, b, ca=1, cb=0):
    return lax.dot_general(a, b, (((ca,), (cb,)), ((), ())), preferred_element_type=F32)


def dot_t(a, b):
    return dot(a, b, 1, 1)


def rotary_tables(tokens):
    rate = float(THETA) ** (-np.arange(HALF, dtype=np.float64) / HALF)
    coarse = np.arange(0, tokens, FINE, dtype=np.float64)[:, None] * rate
    fine = np.arange(FINE, dtype=np.float64)[:, None] * rate
    return [jnp.asarray(f(t), F32) for t in (coarse, fine) for f in (np.cos, np.sin)]


def fill_rotary(tables, cos_s, sin_s):
    ca, sa, cb, sb = (t[...] for t in tables)
    for n in range(ca.shape[0]):
        c, s = ca[n : n + 1, :], sa[n : n + 1, :]
        cos_s[n * FINE : (n + 1) * FINE, :] = c * cb - s * sb
        sin_s[n * FINE : (n + 1) * FINE, :] = s * cb + c * sb


def turn(t, cos, sin):
    out = []
    for at in range(0, t.shape[1], HEAD):
        a, b = t[:, at : at + HALF], t[:, at + HALF : at + HEAD]
        out += [a * cos - b * sin, b * cos + a * sin]
    return jnp.concatenate(out, axis=1)


def norm_of(wide):
    scale = lax.rsqrt(jnp.mean(wide * wide, -1, keepdims=True) + 1e-6)
    return (wide * scale).astype(BF16), scale


def norm_back(by, wide, scale):
    along = jnp.sum(by * wide, -1, keepdims=True) * (1 / wide.shape[1])
    return (scale * by - wide * (scale * scale * scale * along)).astype(BF16)


def rounded(t):
    return t.astype(BF16).astype(F32)


def add(a, b):
    return (a.astype(F32) + b.astype(F32)).astype(BF16)


def diagonal():
    return lax.broadcasted_iota(jnp.int32, (TILE, TILE), 1) >= lax.broadcasted_iota(jnp.int32, (TILE, TILE), 0)


LAG = 2
MESH = pl.DeviceIdType.MESH
UNIT = 512
ROWS = 64
ATT, MLP = NAMES[:4], NAMES[4:]
DMA = pltpu.SemaphoreType.DMA


def to(src, dst, s_sem, r_sem, who):
    return pltpu.make_async_remote_copy(src_ref=src, dst_ref=dst, send_sem=s_sem, recv_sem=r_sem, device_id={"dp": who}, device_id_type=MESH)


def meet(me):
    barrier = pltpu.get_barrier_semaphore()
    for o in range(1, 8):
        pl.semaphore_signal(barrier, inc=1, device_id={"dp": lax.rem(me + o, 8)}, device_id_type=MESH)
    pl.semaphore_wait(barrier, 7)


def sum_scratch(total):
    return [pltpu.VMEM((total, 4, ROWS, UNIT), BF16), pltpu.VMEM((total, 4, ROWS, UNIT), BF16), pltpu.VMEM((total, 5, ROWS, UNIT), BF16),
            DMA((total,)), DMA((total,)), DMA((total,)), DMA((total, 4)), DMA((total, 5))]


class Sum:
    def __init__(self, raw, where, scratch):
        self.raw, self.where, self.total = raw, where, len(where)
        self.ticks = self.total + 3 * LAG
        self.own, self.other, self.came, self.own_sem, self.psend, self.precv, self.send, self.recv = scratch
        self.me = lax.axis_index("dp")
        self.z, self.core = lax.div(self.me, 2), lax.rem(self.me, 2)
        self.partner = 2 * self.z + 1 - self.core
        self.left, self.right = jnp.maximum(self.me - 2, 0), jnp.minimum(self.me + 2, 7)

    def swap(self, n):
        k, at = self.where[n]
        return to(self.raw[k].at[:, 1 - self.core, :, pl.ds(at, UNIT)], self.other.at[n], self.psend.at[n], self.precv.at[n], self.partner)

    def start(self):
        for n, (k, at) in enumerate(self.where):
            pltpu.make_async_copy(self.raw[k].at[:, self.core, :, pl.ds(at, UNIT)], self.own.at[n], self.own_sem.at[n]).start()
        meet(self.me)
        for n in range(self.total):
            self.swap(n).start()

    def both(self, c, t):
        return self.own[c, t].astype(F32) + self.other[c, t].astype(F32)

    def hop(self, c, t, slot, who):
        return to(self.own.at[c, t], self.came.at[c, slot], self.send.at[c, t], self.recv.at[c, slot], who)

    def pass_on(self, c, t, first, slot, who):
        @pl.when(first)
        def _():
            self.own[c, t] = self.both(c, t).astype(BF16)

        @pl.when(jnp.logical_not(first))
        def _():
            self.hop(c, t, t, who).wait_recv()
            self.own[c, t] = (self.both(c, t) + self.came[c, t].astype(F32)).astype(BF16)

        self.hop(c, t, slot, who).start()

    def tick(self, t):
        total, z = self.total, self.z

        @pl.when(t < total)
        def _():
            pltpu.make_async_copy(self.own.at[t], self.own.at[t], self.own_sem.at[t]).wait()
            to(self.own.at[t], self.other.at[t], self.psend.at[t], self.precv.at[t], self.partner).wait_recv()

        c = t - LAG * z

        @pl.when((c >= 0) & (c < total))
        def _():
            for b in (3, 2, 1):
                @pl.when(z < b)
                def _():
                    self.pass_on(c, b, z == 0, b, self.right)

        d = t - LAG * (3 - z)

        @pl.when((d >= 0) & (d < total))
        def _():
            for b in (0, 1, 2):
                @pl.when(z > b)
                def _():
                    self.pass_on(d, b, z == 3, jnp.where(z == b + 1, 4, b), self.left)

        f = t - 3 * LAG

        @pl.when((f >= 0) & (f < total))
        def _():
            @pl.when(z > 0)
            def _():
                self.hop(f, z, z, self.right).wait_recv()

            @pl.when(z < 3)
            def _():
                self.hop(f, z, 4, self.left).wait_recv()

            mine = self.both(f, z)

            @pl.when(z == 0)
            def _():
                self.own[f, z] = (mine + self.came[f, 4].astype(F32)).astype(BF16)

            @pl.when(z == 3)
            def _():
                self.own[f, z] = (mine + self.came[f, z].astype(F32)).astype(BF16)

            @pl.when((z > 0) & (z < 3))
            def _():
                self.own[f, z] = (mine + self.came[f, z].astype(F32) + self.came[f, 4].astype(F32)).astype(BF16)

    def run(self, first):
        lax.fori_loop(first, self.ticks, lambda t, _: self.tick(t), None)

    def drain(self):
        def one(c, _):
            to(self.own.at[c], self.other.at[c], self.psend.at[c], self.precv.at[c], self.partner).wait_send()
            for b in range(4):
                @pl.when(self.z != b)
                def _():
                    self.hop(c, b, b, self.right).wait_send()

        lax.fori_loop(0, self.total, one, None)

    def hand_out(self, out):
        c = pltpu.make_async_copy(self.own.at[:, self.z], out, self.own_sem.at[0])
        c.start()
        c.wait()


def forward_kernel(x_ref, ca, sa, cb, sb, wq, wk, wv, wo, wg, wu, wd, q_out, k_out, v_out, att_out, h1_out, h_out, lse_out,
                   cos_s, sin_s, h_s, k_s, vt_s, top_s, mix_s):
    layer, i = pl.program_id(0), pl.program_id(1)
    heads = wq.shape[2] // HEAD
    e = HEAD**-0.5 * LOG2E
    here = pl.ds(pl.multiple_of(i * TILE, TILE), TILE)

    @pl.when((layer == 0) & (i == 0))
    def _():
        fill_rotary((ca, sa, cb, sb), cos_s, sin_s)
        vt_s[...] = jnp.ones_like(vt_s)

    @pl.when(layer == 0)
    def _():
        h_s[here, :] = x_ref[0]

    h = h_s[here, :]
    h_out[0] = h
    a, _ = norm_of(h.astype(F32))
    cos, sin = cos_s[here, :], sin_s[here, :]
    q = turn(rounded(dot(a, wq[0])), cos, sin).astype(BF16)
    k = turn(rounded(dot(a, wk[0])), cos, sin).astype(BF16)
    v = dot(a, wv[0]).astype(BF16)
    q_out[0], k_out[0], v_out[0] = q, k, v
    k_s[here, :] = k
    vt = v.T
    for n in range(heads):
        vt_s[n, :HEAD, here] = vt[n * HEAD : (n + 1) * HEAD, :]

    top_s[...] = jnp.full_like(top_s, NEG)
    mix_s[...] = jnp.zeros_like(mix_s)

    def scores_of(j):
        return [dot_t(k_s[j * TILE : (j + 1) * TILE, n * HEAD : (n + 1) * HEAD], q_out[0, :, n * HEAD : (n + 1) * HEAD]) for n in range(heads)]

    def blocks(last):
        later = scores_of(0)
        for j in range(last + 1):
            scores, later = later, scores_of(j + 1) if j < last else later
            weights, keeps = [], []
            for n, t in enumerate(scores):
                if j == last:
                    t = jnp.where(diagonal(), t, HIDDEN)
                old = top_s[n : n + 1, :]
                top = jnp.maximum(old, t.max(axis=0, keepdims=True))
                top_s[n : n + 1, :] = top
                weights.append(jnp.exp2((t - top) * e).astype(BF16))
                keeps.append(jnp.exp2((old - top) * e))
            for n in range(heads):
                mix_s[n] = mix_s[n] * keeps[n] + dot(vt_s[n, :, j * TILE : (j + 1) * TILE], weights[n])

    for last in range(k_s.shape[0] // TILE):
        pl.when(i == last)(functools.partial(blocks, last))
    out = []
    for n in range(heads):
        total = mix_s[n, HEAD : HEAD + 1, :]
        out.append((mix_s[n, :HEAD, :] * (1 / total)).T.astype(BF16))
        lse_out[0, n : n + 1, :] = top_s[n : n + 1, :] * e + jnp.log2(total)
    att = jnp.concatenate(out, axis=1)
    att_out[0] = att
    h1 = add(h, dot(att, wo[0]).astype(BF16))
    h1_out[0] = h1

    @pl.when(layer < pl.num_programs(0) - 1)
    def _():
        b, _ = norm_of(h1_out[0].astype(F32))
        total = None
        for at in range(0, wg.shape[2], PART):
            gate, up = dot(b, wg[0, :, at : at + PART]), dot(b, wu[0, :, at : at + PART])
            part = dot((gate * jax.nn.sigmoid(gate) * up).astype(BF16), wd[0, at : at + PART, :])
            total = part if total is None else total + part
        h_s[here, :] = add(h1_out[0], total.astype(BF16))


def forward(x, w):
    layers, d, wide = w["wq"].shape
    tokens, hidden = x.shape[1], w["w_gate"].shape[2]
    assert tokens % TILE == 0 and hidden % PART == 0
    heads = wide // HEAD
    whole = lambda shape: pl.BlockSpec(shape, lambda l, i: (0,) * len(shape))
    each = lambda shape: pl.BlockSpec((1, *shape), lambda l, i: (l, 0, 0))
    most = lambda shape: pl.BlockSpec((1, *shape), lambda l, i: (jnp.minimum(l, layers - 2), 0, 0))
    tile = lambda width: pl.BlockSpec((1, TILE, width), lambda l, i: (l, i, 0))
    tables = rotary_tables(tokens)
    flops = 2 * tokens * (layers * d * wide * 4 + (layers - 1) * 3 * d * hidden + layers * tokens * wide)
    return pl.pallas_call(
        forward_kernel,
        grid=(layers, tokens // TILE),
        in_specs=[pl.BlockSpec((1, TILE, d), lambda l, i: (0, jnp.where(l == 0, i, tokens // TILE - 1), 0)), *(whole(t.shape) for t in tables),
                  each((d, wide)), each((d, wide)), each((d, wide)), each((wide, d)), most((d, hidden)), most((d, hidden)), most((hidden, d))],
        out_specs=[tile(wide)] * 4 + [tile(d)] * 2 + [pl.BlockSpec((1, 8, TILE), lambda l, i: (l, 0, i))],
        out_shape=[jax.ShapeDtypeStruct((layers, tokens, wide), BF16)] * 4 + [jax.ShapeDtypeStruct((layers, tokens, d), BF16)] * 2
        + [jax.ShapeDtypeStruct((layers, 8, tokens), F32)],
        scratch_shapes=[pltpu.VMEM((tokens, HALF), F32), pltpu.VMEM((tokens, HALF), F32), pltpu.VMEM((tokens, d), BF16),
                        pltpu.VMEM((tokens, wide), BF16), pltpu.VMEM((heads, HEAD + 16, tokens), BF16), pltpu.VMEM((8, TILE), F32),
                        pltpu.VMEM((heads, HEAD + 16, TILE), F32)],
        compiler_params=pltpu.CompilerParams(dimension_semantics=("arbitrary", "arbitrary"), vmem_limit_bytes=VMEM),
        cost_estimate=pl.CostEstimate(flops=flops, bytes_accessed=40 * tokens * d, transcendentals=tokens * tokens * heads),
        name="forward",
    )(x, *tables, *(w[n] for n in NAMES))


def mlp_back_kernel(by_ref, h1_ref, wg, wu, wd, by_h1, g_out, dg_s, du_s, dd_s):
    i = pl.program_id(0)
    hidden = wg.shape[2]

    @pl.when(i == 0)
    def _():
        for s in (dg_s, du_s, dd_s):
            s[...] = jnp.zeros_like(s)

    by, wide = by_ref[0], h1_ref[0].astype(F32)
    b, scale = norm_of(wide)
    bt, byt = b.T, by.T
    by_b = [None, None]
    for at in range(0, hidden, PART):
        cut = slice(at, at + PART)
        gate, up = dot(b, wg[0, :, cut]), dot(b, wu[0, :, cut])
        by_p = rounded(dot_t(by, wd[0, cut, :]))
        s = jax.nn.sigmoid(gate)
        act = gate * s
        p = (act * up).astype(BF16)
        by_up = (by_p * act).astype(BF16)
        by_gate = (by_p * up * (s + act * (1 - s))).astype(BF16)
        dd_s[:, cut] += dot(byt, p)
        dg_s[:, cut] += dot(bt, by_gate)
        du_s[:, cut] += dot(bt, by_up)
        parts = dot_t(by_gate, wg[0, :, cut]), dot_t(by_up, wu[0, :, cut])
        by_b = [new if old is None else old + new for old, new in zip(by_b, parts)]
    by_h1[0] = add(by, norm_back(rounded(rounded(by_b[0]) + rounded(by_b[1])), wide, scale))

    @pl.when(i == pl.num_programs(0) - 1)
    def _():
        g_out[:, :hidden] = dg_s[...].astype(BF16)
        g_out[:, hidden : 2 * hidden] = du_s[...].astype(BF16)
        d = by.shape[1]
        ways = d // ROWS
        deep = hidden // ways
        for n in range(ways):
            own = dd_s[:, n * deep : (n + 1) * deep].T.astype(BF16)
            for c in range(deep // ROWS):
                g_out[n * ROWS : (n + 1) * ROWS, 2 * hidden + c * d : 2 * hidden + (c + 1) * d] = own[c * ROWS : (c + 1) * ROWS, :]


def mlp_back(layer, at, by, h1, w):
    layers, d, hidden = w["w_gate"].shape
    tokens = by.shape[1]
    one = lambda shape: pl.BlockSpec((1, *shape), lambda i: (layer, 0, 0), pipeline_mode=pl.Buffered(1))
    tile = lambda n: pl.BlockSpec((1, TILE, d), lambda i: (n, i, 0))
    return pl.pallas_call(
        mlp_back_kernel,
        grid=(tokens // TILE,),
        in_specs=[tile(0), tile(at), one((d, hidden)), one((d, hidden)), one((hidden, d))],
        out_specs=[tile(0), pl.BlockSpec((d, 3 * hidden), lambda i: (0, 0), pipeline_mode=pl.Buffered(1))],
        out_shape=[jax.ShapeDtypeStruct((1, tokens, d), BF16), jax.ShapeDtypeStruct((d, 3 * hidden), BF16)],
        scratch_shapes=[pltpu.VMEM((d, hidden), F32)] * 3,
        compiler_params=pltpu.CompilerParams(dimension_semantics=("arbitrary",), vmem_limit_bytes=VMEM),
        cost_estimate=pl.CostEstimate(flops=16 * tokens * d * hidden, bytes_accessed=20 * tokens * d, transcendentals=tokens * hidden),
        name="mlp_back",
    )(by, h1, w["w_gate"], w["w_up"], w["w_down"])


def att_back_kernel(more, by_ref, h_ref, q_ref, k_ref, v_ref, att_ref, lse_ref, ca, sa, cb, sb, wq, wk, wv, wo, *rest):
    by_h, rest = (rest[0], rest[1:]) if more else (None, rest)
    g_out, cos_s, sin_s, dq_s, dk_s, dv_s, g_s, do_s, delta_s = rest
    step = pl.program_id(0)
    i = pl.num_programs(0) - 1 - step
    d, full = wq.shape[1], wq.shape[2]
    heads = full // HEAD
    scale = HEAD**-0.5
    e = scale * LOG2E
    here = pl.ds(pl.multiple_of(i * TILE, TILE), TILE)

    @pl.when(step == 0)
    def _():
        fill_rotary((ca, sa, cb, sb), cos_s, sin_s)
        for s in (dk_s, dv_s, g_s):
            s[...] = jnp.zeros_like(s)

    by = by_ref[0]
    by_att = dot_t(by, wo[0]).astype(BF16)
    do_s[...] = by_att
    att = att_ref[0]
    g_s[3] += dot(att.T, by)
    rows = by_att.astype(F32) * att.astype(F32)
    for n in range(heads):
        delta_s[n : n + 1, :] = rows[:, n * HEAD : (n + 1) * HEAD].T.sum(axis=0, keepdims=True)
    dq_s[...] = jnp.zeros_like(dq_s)

    def block(j, masked):
        at = pl.ds(pl.multiple_of(j * TILE, TILE), TILE)
        cuts = [slice(n * HEAD, (n + 1) * HEAD) for n in range(heads)]
        qs = [q_ref[0, :, c] for c in cuts]
        dos = [do_s[:, c] for c in cuts]
        scores = [dot_t(k_ref[0, at, c], qs[n]) for n, c in enumerate(cuts)]
        dps = [dot_t(v_ref[0, at, c], dos[n]) for n, c in enumerate(cuts)]
        for n, c in enumerate(cuts):
            p = jnp.exp2(scores[n] * e - lse_ref[0, n : n + 1, :])
            if masked:
                p = jnp.where(diagonal(), p, 0.0)
            ds = (p * (dps[n] - delta_s[n : n + 1, :])).astype(BF16)
            dv_s[at, c] += dot(p.astype(BF16), dos[n])
            dk_s[at, c] += dot(ds, qs[n])
            dq_s[n] += dot(k_ref[0, at, c].T, ds)

    lax.fori_loop(0, i, lambda j, _: block(j, False), None)
    block(i, True)

    cos, sin = cos_s[here, :], -sin_s[here, :]
    dq = jnp.concatenate([(dq_s[n] * scale).T for n in range(heads)], axis=1)
    dq = turn(rounded(dq), cos, sin).astype(BF16)
    dk = turn(rounded(dk_s[here, :] * scale), cos, sin).astype(BF16)
    dv = dv_s[here, :].astype(BF16)
    wide = h_ref[0].astype(F32)
    a, size = norm_of(wide)
    at = a.T
    for n, t in enumerate((dq, dk, dv)):
        g_s[n] += dot(at, t)
    if more:
        by_a = sum(rounded(dot_t(t, m[0])) for t, m in ((dq, wq), (dk, wk), (dv, wv)))
        by_h[0] = add(by, norm_back(rounded(by_a), wide, size))

    @pl.when(step == pl.num_programs(0) - 1)
    def _():
        for n in range(4):
            g_out[:, n * full : (n + 1) * full] = g_s[n].astype(BF16)


def att_back(layer, by, kept, w, more):
    q, k, v, att, _, h, lse = kept
    layers, d, full = w["wq"].shape
    assert d == full
    tokens = by.shape[1]
    last = tokens // TILE - 1
    heads = full // HEAD
    whole = lambda shape: pl.BlockSpec(shape, lambda i: (0,) * len(shape))
    one = lambda shape: pl.BlockSpec((1, *shape), lambda i: (layer, 0, 0), pipeline_mode=pl.Buffered(1))
    tile = lambda n: pl.BlockSpec((1, TILE, d), lambda i: (n, last - i, 0))
    tables = rotary_tables(tokens)
    return pl.pallas_call(
        functools.partial(att_back_kernel, more),
        grid=(tokens // TILE,),
        in_specs=[tile(0), tile(layer), tile(layer), one((tokens, full)), one((tokens, full)), tile(layer),
                  pl.BlockSpec((1, 8, TILE), lambda i: (layer, 0, last - i)), *(whole(t.shape) for t in tables),
                  one((d, full)), one((d, full)), one((d, full)), one((full, d))],
        out_specs=[tile(0)] * more + [pl.BlockSpec((d, 4 * full), lambda i: (0, 0), pipeline_mode=pl.Buffered(1))],
        out_shape=[jax.ShapeDtypeStruct((1, tokens, d), BF16)] * more + [jax.ShapeDtypeStruct((d, 4 * full), BF16)],
        scratch_shapes=[pltpu.VMEM((tokens, HALF), F32), pltpu.VMEM((tokens, HALF), F32), pltpu.VMEM((heads, HEAD, TILE), F32),
                        pltpu.VMEM((tokens, full), F32), pltpu.VMEM((tokens, full), F32), pltpu.VMEM((4, d, full), F32),
                        pltpu.VMEM((TILE, full), BF16), pltpu.VMEM((8, TILE), F32)],
        compiler_params=pltpu.CompilerParams(dimension_semantics=("arbitrary",), vmem_limit_bytes=VMEM),
        cost_estimate=pl.CostEstimate(flops=2 * tokens * d * (8 * d + 3 * tokens), bytes_accessed=20 * tokens * d, transcendentals=tokens * tokens * heads // 2),
        name="att_back",
    )(by, h, q, k, v, att, lse, *tables, w["wq"], w["wk"], w["wv"], w["wo"])


def sum_kernel(where, *refs):
    refs = list(refs)
    raw = [refs.pop(0) for _ in range(1 + max(n for n, _ in where))]
    out = refs.pop(0)
    work = Sum(raw, where, refs)
    work.start()
    work.run(0)
    work.drain()
    work.hand_out(out)


def summed(gradients):
    where = tuple((i, at) for i, g in enumerate(gradients) for at in range(0, g.shape[1], UNIT))
    operands = [g.reshape(4, 2, ROWS, -1) for g in gradients]
    any_ = pl.BlockSpec(memory_space=pl.ANY)
    return pl.pallas_call(
        functools.partial(sum_kernel, where),
        in_specs=[any_] * len(operands),
        out_specs=any_,
        out_shape=jax.ShapeDtypeStruct((len(where), ROWS, UNIT), BF16),
        scratch_shapes=sum_scratch(len(where)),
        compiler_params=pltpu.CompilerParams(collective_id=1, has_side_effects=True, vmem_limit_bytes=VMEM),
        cost_estimate=pl.CostEstimate(flops=int(5e10), bytes_accessed=int(1e7), transcendentals=0),
        name="summed",
    )(*operands)


def units_of(names, m_shapes):
    out = []
    for name in names:
        _, rows, width = m_shapes[name]
        out += [(name, r, c) for r in range(0, rows, ROWS) for c in range(0, width, UNIT)]
    return out


def finish_kernel(blocks, units, shapes, count, *refs):
    refs = list(refs)
    take = lambda n: [refs.pop(0) for _ in range(n)]
    done = take(len(blocks))
    w, m, v, new = (dict(zip(NAMES, take(7))) for _ in range(4))
    g_out, factor_out = take(2)
    ws, ns, ms, vs = (dict(zip(NAMES, take(7))) for _ in range(4))
    (g_s, part, parts, factor_s, done_sem, load_sem, store_sem, nsend, nrecv, asend, arecv) = refs
    me = lax.axis_index("dp")
    z, core = lax.div(me, 2), lax.rem(me, 2)
    partner = 2 * z + 1 - core
    left, right = jnp.maximum(me - 2, 0), jnp.minimum(me + 2, 7)
    layers = shapes["wq"][0]

    loads = []
    for ref, (start, n, at) in zip(done, blocks):
        if len(ref.shape) == 3:
            loads.append(pltpu.make_async_copy(ref.at[pl.ds(start, n)], g_s.at[pl.ds(at, n)], done_sem.at[at]))
        else:
            loads += [pltpu.make_async_copy(ref.at[:, pl.ds(start + i * UNIT, UNIT)], g_s.at[at + i], done_sem.at[at + i]) for i in range(n)]
    for i, name in enumerate(NAMES):
        rows = shapes[name][1]
        loads.append(pltpu.make_async_copy(w[name].at[:, pl.ds(pl.multiple_of(me * rows, ROWS), rows), :], ws[name], load_sem.at[0, i]))
        loads.append(pltpu.make_async_copy(m[name], ms[name], load_sem.at[1, i]))
        loads.append(pltpu.make_async_copy(v[name], vs[name], load_sem.at[2, i]))
    for c in loads:
        c.start()
    meet(me)
    for c in loads[: -3 * len(NAMES)]:
        c.wait()

    def squares(n, sofar):
        g = g_s[n].astype(F32)
        return sofar + g * g

    size = lax.fori_loop(0, len(units), squares, jnp.zeros((ROWS, UNIT), F32))
    part[...] = jnp.broadcast_to(jnp.sum(size, keepdims=True), part.shape)
    parts[me] = part[...]
    tell = [to(part, parts.at[me], nsend.at[o], nrecv.at[o], lax.rem(me + o, 8)) for o in range(1, 8)]
    for c in tell:
        c.start()
    for c in loads[-3 * len(NAMES) :]:
        c.wait()
    for c in tell:
        c.wait_recv()
    size = parts[0]
    for o in range(1, 8):
        size = size + parts[o]
    factor_s[...] = jnp.minimum(1.0, 0.5 * lax.rsqrt(size / count + 1e-30))
    factor = factor_s[:1, :1]

    pieces = [(name, layer) for names in (MLP, ATT) for layer in range(layers) for name in names]

    def region(ref, name, layer, chip, c):
        rows = shapes[name][1]
        return ref[name].at[layer, pl.ds(pl.multiple_of((2 * chip + c) * rows, ROWS), rows), :]

    def share(p, slot, chip, first, who, core_of):
        name, layer = pieces[p]
        there = region(new, name, layer, chip, core_of)
        src = ns[name].at[layer] if first else there
        return to(src, there, asend.at[slot, p], arecv.at[slot, p], who)

    stores = [pltpu.make_async_copy(g_s, g_out, store_sem.at[len(pieces)]), pltpu.make_async_copy(factor_s, factor_out, store_sem.at[len(pieces) + 1])]
    for p in range(len(pieces) + 3):
        if p < len(pieces):
            name, layer = pieces[p]
            for u, (uname, ulayer, r, c) in enumerate(units):
                if (uname, ulayer) != (name, layer):
                    continue
                at = (layer, slice(r, r + ROWS), slice(c, c + UNIT))
                ns[name][at] = adamw(ws[name][at].astype(F32), ms[name][at], vs[name][at], g_s[u].astype(F32) * factor)[0]

            @pl.when(z < 3)
            def _():
                share(p, 1, z, True, right, core).start()

            @pl.when(z > 0)
            def _():
                share(p, 4, z, True, left, core).start()

            share(p, 0, z, True, partner, core).start()
            stores.append(pltpu.make_async_copy(ns[name].at[layer], region(new, name, layer, z, core), store_sem.at[p]))
            stores[-1].start()
            if p == 0:
                for c in stores[:2]:
                    c.start()
        for far in (1, 2, 3):
            q = p - far
            if not 0 <= q < len(pieces):
                continue

            @pl.when(z >= far)
            def _():
                share(q, far, z - far, False, right, core).wait_recv()
                if far < 3:
                    @pl.when(z < 3)
                    def _():
                        share(q, far + 1, z - far, False, right, core).start()
                share(q, 6 + far, z - far, False, partner, core).start()

            @pl.when(z <= 3 - far)
            def _():
                share(q, 3 + far, z + far, False, left, core).wait_recv()
                if far < 3:
                    @pl.when(z > 0)
                    def _():
                        share(q, 4 + far, z + far, False, left, core).start()
                share(q, 9 + far, z + far, False, partner, core).start()

    for c in tell:
        c.wait_send()
    for p in range(len(pieces)):
        mine, theirs = share(p, 0, z, True, partner, core), share(p, 0, z, False, partner, 1 - core)
        mine.wait_send()
        theirs.wait_recv()

        @pl.when(z < 3)
        def _():
            share(p, 1, z, True, right, core).wait_send()

        @pl.when(z > 0)
        def _():
            share(p, 4, z, True, left, core).wait_send()

        for far in (1, 2, 3):
            @pl.when(z >= far)
            def _():
                if far < 3:
                    @pl.when(z < 3)
                    def _():
                        share(p, far + 1, z - far, False, right, core).wait_send()
                share(p, 6 + far, z - far, False, partner, core).wait_send()
                share(p, 6 + far, z - far, False, partner, 1 - core).wait_recv()

            @pl.when(z <= 3 - far)
            def _():
                if far < 3:
                    @pl.when(z > 0)
                    def _():
                        share(p, 4 + far, z + far, False, left, core).wait_send()
                share(p, 9 + far, z + far, False, partner, core).wait_send()
                share(p, 9 + far, z + far, False, partner, 1 - core).wait_recv()
    for c in stores:
        c.wait()


def adamw(w, m, v, g):
    m = 0.9 * m + 0.1 * g
    v = 0.95 * v + 0.05 * g * g
    return (w - 0.02 * (m * lax.rsqrt(v + 1e-8) + 0.1 * w)).astype(BF16), m, v


CUTS = 4


def results_kernel(units, g_ref, factor_ref, *refs):
    w, m, v, w_out, m_out, v_out = (dict(zip(NAMES, refs[i : i + 7])) for i in range(0, 42, 7))
    layer, cut = pl.program_id(0), pl.program_id(1)
    factor = factor_ref[:1, :1]
    for name in NAMES:
        w_out[name][...] = w[name][...]
    first = layer * len(units)

    for n, (name, r, c) in enumerate(units):
        rows = m[name].shape[1]
        here = (0, slice(0, rows), slice(c, c + UNIT))

        def do(g):
            _, m_out[name][here], v_out[name][here] = adamw(0.0, m[name][here], v[name][here], g.astype(F32) * factor)

        if rows == ROWS:
            @pl.when(cut == r // ROWS)
            def _():
                do(g_ref[first + n])
        else:
            do(g_ref[first + n, pl.ds(pl.multiple_of(cut * rows, rows), rows), :])


def results(units, g, factor, w, m, v):
    cut = lambda one: pl.BlockSpec((1, one.shape[1] // CUTS, one.shape[2]), lambda l, i: (l, i, 0))
    whole = lambda a: pl.BlockSpec(a.shape, lambda l, i: (0,) * a.ndim)
    arrays = (*w, *m, *v)
    return pl.pallas_call(
        functools.partial(results_kernel, units),
        grid=(m[0].shape[0], CUTS),
        in_specs=[whole(g), whole(factor), *(cut(a) for a in arrays)],
        out_specs=[cut(a) for a in arrays],
        out_shape=[jax.ShapeDtypeStruct(a.shape, a.dtype) for a in arrays],
        compiler_params=pltpu.CompilerParams(dimension_semantics=("arbitrary", "arbitrary"), vmem_limit_bytes=VMEM),
        cost_estimate=pl.CostEstimate(flops=int(1e7), bytes_accessed=int(5e7), transcendentals=0),
        name="results",
    )(g, factor, *arrays)


def finish(groups, weights, m, v):
    shapes = {name: one.shape for name, one in zip(NAMES, m, strict=True)}
    in_layer = units_of(NAMES, shapes)
    layers = m[0].shape[0]
    units = [(name, layer, r, c) for layer in range(layers) for name, r, c in in_layer]
    blocks = [(start, len(units_of(names, shapes)), units.index((names[0], layer, 0, 0))) for _, start, layer, names in groups]
    count = 8 * sum(one.size for one in m)
    any_ = pl.BlockSpec(memory_space=pl.ANY)
    pieces = 7 * layers
    vmem = lambda dtype: [pltpu.VMEM(one.shape, dtype) for one in m]
    operands = [g for g, *_ in groups] + [*weights, *m, *v]
    g_shape, factor_shape = (len(units), ROWS, UNIT), (8, 128)
    *new, g, factor = pl.pallas_call(
        functools.partial(finish_kernel, blocks, units, shapes, count),
        in_specs=[any_] * len(operands),
        out_specs=[any_] * 9,
        out_shape=[jax.ShapeDtypeStruct(one.shape, BF16) for one in weights]
        + [jax.ShapeDtypeStruct(g_shape, BF16), jax.ShapeDtypeStruct(factor_shape, F32)],
        scratch_shapes=vmem(BF16) + vmem(BF16) + vmem(F32) + vmem(F32) + [
            pltpu.VMEM(g_shape, BF16), pltpu.VMEM((8, 128), F32), pltpu.VMEM((8, 8, 128), F32), pltpu.VMEM(factor_shape, F32),
            DMA((len(units),)), DMA((3, 7)), DMA((pieces + 2,)), DMA((8,)), DMA((8,)), DMA((13, pieces)), DMA((13, pieces))],
        compiler_params=pltpu.CompilerParams(collective_id=2, has_side_effects=True, vmem_limit_bytes=VMEM),
        cost_estimate=pl.CostEstimate(flops=int(1e9), bytes_accessed=int(1e8), transcendentals=0),
        name="finish",
    )(*operands)
    return results(in_layer, g, factor, new, m, v)


def solution(mesh):
    def step(x, dy, *arrays):
        weights, m, v = (arrays[i : i + 7] for i in (0, 7, 14))
        w = dict(zip(NAMES, weights, strict=True))
        layers, d, _ = w["w_gate"].shape
        assert d == ROWS * lax.axis_size("dp") and lax.axis_size("dp") == 8
        kept = forward(x, w)
        by, groups, late = dy, [], []
        for n in reversed(range(layers)):
            by_h1, mlp = mlp_back(n, n, by, kept[4], w)
            groups.append((lax.psum_scatter(mlp, "dp", scatter_dimension=0, tiled=True), 0, n, MLP))
            *by_h, att = att_back(n, by_h1, kept, w, n > 0)
            late.append((att, n))
            by = by_h[0] if by_h else by
        blocks = summed([att for att, _ in late])
        groups += [(blocks, i * len(ATT), n, ATT) for i, (_, n) in enumerate(late)]
        return tuple(finish(groups, weights, m, v))

    states, all_of, cut = P(("rep", "dp"), None, None), P(None, None, None), P(None, "dp", None)
    return jax.shard_map(
        step,
        mesh=mesh,
        in_specs=(states, states) + (all_of,) * 7 + (cut,) * 14,
        out_specs=(P("rep", None, None),) * 7 + (P("rep", "dp", None),) * 14,
        check_vma=False,
    )
```
